256 devices in a mesh: seq: 4 (over y), tp: 8 (over z), grp: 8 (over x, core).
Axes of the slice: x: 4, y: 4, z: 8, core: 2. Of those that a mesh axis runs over, the one named last changes fastest.
Arguments:
- queries: bfloat16 [16, 64, 128], P('grp', 'tp'), may hold values from -2000 to 2000
- cache_pool: bfloat16 [2048, 8, 2, 128, 128], P(('seq', 'grp'), 'tp'), may hold values from -6 to 6
- block_scale: bfloat16 [2048, 8, 2], P(('seq', 'grp'), 'tp'), may hold values from 0.29 to 3
- block_table: int32 [16, 128], replicated, may hold values from 0 to 2047, as said below
- lengths: int32 [16], replicated, may hold values from 128 to 16384
- output_weight: bfloat16 [8192, 8192], P('tp', ('seq', 'grp')), may hold values from -0.0625 to 0.0625
Outputs:
- attention_output: bfloat16 [16, 8192], P('tp', ('seq', 'grp'))
- decode_cache: bfloat16 [16, 128, 8, 2, 128, 128], P('grp', 'seq', 'tp')
- decode_scale: bfloat16 [16, 128, 8, 2], P('grp', 'seq', 'tp')
The draws below stay inside these ranges and needn't reach their ends.
Inputs may be any that keep to these rules, and one draw needn't show every extreme that they name: block_table names every pool slot exactly once. Take any run of 64 slots starting at a multiple of 64, any group of 2 consecutive requests starting at a multiple of 2, and any range of 32 block positions starting at a multiple of 32: exactly 2 slots of the run hold blocks of those requests at those positions.
All inputs are finite; a program needn't handle non-finite values.
Results may differ from the reference program's by a relative error of at most 0.014.
Values may be sent and summed in bfloat16 or wider, within the bound.
A program may use at most 64 MiB of HBM per device.

```python
import math
import jax
import jax.numpy as jnp
from jax import lax

D = 8192
H = 64
KVH = 8
HD = 128
BLK = 128
NB = 128
BPG = 2
BATCH = 16
POOL = 2048
POOL_DEV = 64
NBQ = 32
CAP = 2
N_SEQ = 4
N_GRP = 8


def block_layout(key):
    base_key = jax.random.fold_in(key, 7)
    pair_keys = jax.random.split(jax.random.fold_in(base_key, 1), N_GRP * N_SEQ)
    spread = jax.vmap(lambda sub_key: jax.random.permutation(sub_key, BPG * NBQ))(pair_keys).astype(jnp.int32)
    owner_keys = jax.random.split(jax.random.fold_in(base_key, 2), N_SEQ * N_GRP)
    places = jax.vmap(lambda sub_key: jax.random.permutation(sub_key, POOL_DEV))(owner_keys).astype(jnp.int32)
    owners = spread // CAP
    within = spread % CAP
    pair_ids = jnp.arange(N_GRP * N_SEQ, dtype=jnp.int32)[:, None]
    column = pair_ids * CAP + within
    slot_ids = owners * POOL_DEV + places[owners, column]
    return slot_ids.reshape(N_GRP, N_SEQ, BPG, NBQ).transpose(0, 2, 1, 3).reshape(BATCH, NB).astype(jnp.int32)


def cache_law(key):
    base_key = jax.random.fold_in(key, 13)
    pool_shape = (POOL, KVH, 2, BLK, HD)
    pool_data = jnp.clip(jax.random.normal(jax.random.fold_in(base_key, 1), pool_shape, jnp.float32), -6.0, 6.0)
    scale_data = jnp.exp(jax.random.uniform(jax.random.fold_in(base_key, 2), (POOL, KVH, 2), jnp.float32, math.log(0.5), math.log(2.0)))
    query_data = jnp.clip(2.5 * jax.random.normal(jax.random.fold_in(base_key, 3), (BATCH, H, HD), jnp.float32), -15.0, 15.0)
    return (pool_data, scale_data, query_data)


def draw_queries(key, part):
    return cache_law(key)[2].astype(jnp.bfloat16)


def draw_cache_pool(key, part):
    return cache_law(key)[0].astype(jnp.bfloat16)


def draw_block_scale(key, part):
    return cache_law(key)[1].astype(jnp.bfloat16)


def draw_block_table(key, part):
    return block_layout(key)


def set_ends(drawn, rng, smallest, high):
    spot = [jax.random.randint(jax.random.fold_in(rng, axis), (), 0, length) for axis, length in enumerate(drawn.shape)]
    widest = drawn.shape.index(max(drawn.shape))
    beside = spot[:widest] + [(spot[widest] + 1) % drawn.shape[widest]] + spot[widest + 1:]
    return drawn.at[tuple(spot)].set(smallest).at[tuple(beside)].set(high)


def level_of(own_key, shape, cuts, least, largest):
    def one(position, blocks):
        steps = jax.random.uniform(jax.random.fold_in(jax.random.fold_in(own_key, 6), position), (blocks,), jnp.float32, least / len(cuts), largest / len(cuts))
        return jnp.repeat(jnp.exp(steps), shape[position] // blocks).reshape((-1,) + (1,) * (len(shape) - position - 1))

    factor_of = one(*cuts[0])
    for cut in cuts[1:]:
        factor_of = factor_of * one(*cut)
    return factor_of


def gaussian(rng, extent, deviation, most, cuts=(), held_as=jnp.bfloat16):
    array = deviation * jax.random.normal(rng, extent, jnp.float32)
    if cuts:
        array = array * level_of(rng, extent, cuts, -0.22, 0.18)
    return jnp.clip(array, -most, most).astype(held_as)


def setup_inputs(seed: int = 0) -> dict:
    key_list = jax.random.split(jax.random.key(seed), 7)
    return {
        "queries": draw_queries(jax.random.fold_in(key_list[6], 71), 0),
        "cache_pool": draw_cache_pool(jax.random.fold_in(key_list[6], 71), 0),
        "block_scale": draw_block_scale(jax.random.fold_in(key_list[6], 71), 0),
        "block_table": draw_block_table(jax.random.fold_in(key_list[6], 71), 0),
        "lengths": set_ends(jax.random.randint(key_list[4], (BATCH,), BLK, NB * BLK + 1), jax.random.fold_in(key_list[4], 1), BLK, NB * BLK).astype(jnp.int32),
        "output_weight": gaussian(key_list[5], (H * HD, D), (H * HD) ** -0.5, 0.0625, ((0, 8), (1, 32))),
    }


def reference(queries, cache_pool, block_scale, block_table, lengths, output_weight):
    decode_cache = cache_pool[block_table]
    decode_scale = block_scale[block_table]
    groups = H // KVH
    root_scale = 1.0 / math.sqrt(HD)
    offsets = jnp.arange(NB * BLK, dtype=jnp.int32).reshape(NB, BLK)

    def one_request(request_items):
        query_rows, blocks, scales, length = request_items
        key_rows = blocks[:, :, 0].astype(jnp.float32)
        value_rows = blocks[:, :, 1].astype(jnp.float32)
        head_rows = query_rows.reshape(KVH, groups, HD).astype(jnp.float32)
        scores = jnp.einsum('kgd,nktd->nkgt', head_rows, key_rows, precision=lax.Precision.HIGHEST)
        scores = scores * scales[:, :, 0].astype(jnp.float32)[:, :, None, None] * root_scale
        live_mask = (offsets < length)[:, None, None, :]
        scores = jnp.where(live_mask, scores, -jnp.inf)
        peak = lax.optimization_barrier(jnp.max(scores, axis=(0, 3)))
        weight = jnp.where(live_mask, jnp.exp(scores - peak[None, :, :, None]), 0.0)
        denominator = lax.optimization_barrier(jnp.sum(weight, axis=(0, 3)))
        scaled = (weight * scales[:, :, 1].astype(jnp.float32)[:, :, None, None]).astype(jnp.bfloat16)
        numerator = jnp.einsum('nkgt,nktd->kgd', scaled.astype(jnp.float32), value_rows, precision=lax.Precision.HIGHEST)
        return (numerator / denominator[:, :, None]).astype(jnp.bfloat16).reshape(H * HD)
    attended = lax.map(one_request, (queries, decode_cache, decode_scale, lengths))
    attention_output = jnp.dot(attended, output_weight, preferred_element_type=jnp.float32).astype(jnp.bfloat16)
    return (attention_output, decode_cache, decode_scale)
```

```python
import functools
import math

import jax
import jax.numpy as jnp
from jax import lax
from jax.experimental import pallas as pl
from jax.experimental.pallas import tpu as pltpu
from jax.sharding import PartitionSpec as P

MESH = pl.DeviceIdType.MESH
ABSENT = -1e30
NSEQ, NTP, NGRP = 4, 8, 8
NDEV = NSEQ * NGRP
BLK = 128
ROOT = 1.0 / math.sqrt(128.0)
START = (0, 256, 128, 384)


def spread(i):
    turn, rest = i // 8, i % 8
    dy, dc = rest // 2, rest % 2
    return dy, (dy + turn) % 4, dc


def exchange_kernel(
    idx, scal, pool_hbm, q_ref, w_hbm, place_ref,
    arr, out_ref, scale_out,
    pool_k, pool_v, send, qall, w, pmsg, part, amsg, att, pout, zbuf,
    pool_sem, w_sem, q_ssem, q_rsem, b_ssem, b_rsem, p_ssem, p_rsem, a_ssem, a_rsem, z_ssem, z_rsem,
):
    y = lax.axis_index("seq")
    z = lax.axis_index("tp")
    g = lax.axis_index("grp")
    me = y * NGRP + g

    def peer(i):
        dy, dx, dc = spread(i)
        ty = (y + dy) % 4
        tg = ((g // 2 + dx) % 4) * 2 + (g + dc) % 2
        return ty, tg

    barrier = pltpu.get_barrier_semaphore()

    def greet(i, carry):
        ty, tg = peer(i)
        pl.semaphore_signal(barrier, inc=1, device_id={"seq": ty, "grp": tg}, device_id_type=MESH)
        return carry

    lax.fori_loop(1, NDEV, greet, 0)

    def greet_z(i, carry):
        pl.semaphore_signal(barrier, inc=1, device_id={"tp": (z + i) % NTP}, device_id_type=MESH)
        return carry

    lax.fori_loop(1, NTP, greet_z, 0)

    keys_in = pltpu.make_async_copy(pool_hbm.at[:, pl.ds(0, BLK)], pool_k, pool_sem.at[0])
    vals_in = pltpu.make_async_copy(pool_hbm.at[:, pl.ds(BLK, BLK)], pool_v, pool_sem.at[1])
    w_in = pltpu.make_async_copy(w_hbm, w, w_sem)
    keys_in.start()
    vals_in.start()
    w_in.start()
    qall[g] = q_ref[...]

    def pick(c):
        pool, r = (pool_k, pool_v)[c // 2], c % 2

        def body(t, carry):
            slot = idx[2 * t + r]
            send[t, pl.ds(START[c], BLK), :] = pool[slot]
            return carry

        lax.fori_loop(0, NDEV, body, 0)

    def block_copy(c, i):
        ty, tg = peer(i)
        rows = pl.ds(START[c], BLK)
        return pltpu.make_async_remote_copy(
            src_ref=send.at[ty * NGRP + tg, rows],
            dst_ref=arr.at[me, rows],
            send_sem=b_ssem.at[c, i],
            recv_sem=b_rsem.at[c, i],
            device_id={"seq": ty, "grp": tg},
            device_id_type=MESH,
        )

    def send_wave(c):
        def body(i, carry):
            block_copy(c, i).start()
            return carry

        lax.fori_loop(1, NDEV, body, 0)

    def q_copy(i):
        tg = (g + i) % NGRP
        return pltpu.make_async_remote_copy(
            src_ref=q_ref, dst_ref=qall.at[g], send_sem=q_ssem.at[i], recv_sem=q_rsem.at[i],
            device_id={"grp": tg}, device_id_type=MESH,
        )

    keys_in.wait()
    pick(0)
    pl.semaphore_wait(barrier, NDEV - 1 + NTP - 1)
    for i in range(1, NGRP):
        q_copy(i).start()
    send_wave(0)
    pick(1)
    vals_in.wait()
    pick(2)
    pick(3)
    for i in range(1, NGRP):
        q_copy(i).wait()

    row16 = lax.broadcasted_iota(jnp.int32, (16, BLK), 0)
    lane16 = lax.broadcasted_iota(jnp.int32, (16, BLK), 1)
    row4 = lax.broadcasted_iota(jnp.int32, (4, BLK), 0)
    lane4 = lax.broadcasted_iota(jnp.int32, (4, BLK), 1)

    def attend(gg, carry):
        q = qall[gg]
        scores, masks = [], []
        for n in range(8):
            t, r = (n // 2) * NGRP + gg, n % 2
            k = 2 * t + r
            keys = send[t, pl.ds(r * 256, BLK), :]
            s = lax.dot_general(q, keys, (((1,), (1,)), ((), ())), preferred_element_type=jnp.float32)
            s = s * (scal[k] * ROOT)
            limit = jnp.where(row16 < 8, idx[64 + k], idx[128 + k])
            live = lane16 < limit
            scores.append(jnp.where(live, s, ABSENT))
            masks.append(live)
        top = functools.reduce(jnp.maximum, scores)
        peak = jnp.max(top, axis=1, keepdims=True)
        total = jnp.zeros((16, BLK), jnp.float32)
        acc = jnp.zeros((16, BLK), jnp.float32)
        for n in range(8):
            t, r = (n // 2) * NGRP + gg, n % 2
            k = 2 * t + r
            weight = jnp.where(masks[n], jnp.exp(scores[n] - peak), 0.0)
            total = total + weight
            scaled = (weight * scal[64 + k]).astype(jnp.bfloat16)
            acc = acc + jnp.dot(scaled, send[t, pl.ds(r * 256 + BLK, BLK), :], preferred_element_type=jnp.float32)
        denom = jnp.sum(total, axis=1, keepdims=True)
        stats = jnp.where(lane16 == 2, peak, jnp.where(lane16 == 3, denom, 0.0))
        for qq in range(NSEQ):
            t = qq * NGRP + gg
            pmsg[t, pl.ds(0, 4), :] = acc[4 * qq : 4 * qq + 4]
            low = stats[4 * qq : 4 * qq + 4]
            for r in range(2):
                k = 2 * t + r
                low = jnp.where((row4 == r) & (lane4 == 0), scal[k], low)
                low = jnp.where((row4 == r) & (lane4 == 1), scal[64 + k], low)
            pmsg[t, pl.ds(4, 4), :] = low
        return carry

    lax.fori_loop(0, NGRP, attend, 0)

    def p_copy(i):
        ty, tg = peer(i)
        return pltpu.make_async_remote_copy(
            src_ref=pmsg.at[ty * NGRP + tg], dst_ref=part.at[me],
            send_sem=p_ssem.at[i], recv_sem=p_rsem.at[i],
            device_id={"seq": ty, "grp": tg}, device_id_type=MESH,
        )

    def a_copy(i):
        ty, tg = peer(i)
        return pltpu.make_async_remote_copy(
            src_ref=amsg, dst_ref=att.at[(y % 2) * 16 + g * 2 + y // 2],
            send_sem=a_ssem.at[i], recv_sem=a_rsem.at[i],
            device_id={"seq": ty, "grp": tg}, device_id_type=MESH,
        )

    def each(make, what, first, last):
        def body(i, carry):
            getattr(make(i), what)()
            return carry

        lax.fori_loop(first, last, body, 0)

    each(p_copy, "start", 1, NDEV)
    part[me] = pmsg[me]
    send_wave(1)
    each(p_copy, "wait", 1, NDEV)

    peaks = part[:, pl.ds(4, 4), 2:3]
    sums = part[:, pl.ds(4, 4), 3:4]
    peak = jnp.max(peaks, axis=0, keepdims=True)
    factor = jnp.exp(peaks - peak)
    denom = jnp.sum(sums * factor, axis=0)
    numer = jnp.sum(part[:, pl.ds(0, 4), :] * factor, axis=0)
    rows = (numer / denom).astype(jnp.bfloat16).astype(jnp.float32)
    amsg[...] = rows
    att[(y % 2) * 16 + g * 2 + y // 2] = rows
    lanes = lax.broadcasted_iota(jnp.int32, (64, 256), 1)
    at = place_ref[...]
    hot = (lanes == (at // 2) * 8 + 4 + at % 2).astype(jnp.float32).astype(jnp.bfloat16)
    picked = jnp.dot(hot, part[...].reshape(256, BLK).astype(jnp.bfloat16), preferred_element_type=jnp.float32)
    scale_out[...] = picked[:, 0:2].astype(jnp.bfloat16)

    each(a_copy, "start", 1, NDEV)
    send_wave(2)
    send_wave(3)
    arr[me] = send[me]
    w_in.wait()
    each(a_copy, "wait", 1, NDEV)

    total = jnp.zeros((16, 256), jnp.float32)
    for h in range(8):
        lhs = att[pl.ds((h // 4) * 16, 16), h % 4, :].astype(jnp.bfloat16)
        total = total + jnp.dot(lhs, w[pl.ds(h * BLK, BLK), :], preferred_element_type=jnp.float32)
    for k in range(NTP):
        pout[k] = total[2 * k : 2 * k + 2]

    def z_copy(i):
        tz = (z + i) % NTP
        return pltpu.make_async_remote_copy(
            src_ref=pout.at[tz], dst_ref=zbuf.at[z], send_sem=z_ssem.at[i], recv_sem=z_rsem.at[i],
            device_id={"tp": tz}, device_id_type=MESH,
        )

    each(z_copy, "start", 1, NTP)
    zbuf[z] = pout[z]
    each(z_copy, "wait", 1, NTP)
    out_ref[...] = jnp.sum(zbuf[...], axis=0).astype(jnp.bfloat16)

    for c in range(4):
        each(functools.partial(block_copy, c), "wait", 1, NDEV)


def place_kernel(src, arr, out, sem):
    for p in range(64):
        pltpu.make_async_copy(arr.at[src[p]], out.at[p], sem).start()
    pltpu.make_async_copy(arr, out, sem).wait()


def per_device(queries, cache_pool, block_scale, block_table, lengths, output_weight):
    y = lax.axis_index("seq")
    g = lax.axis_index("grp")
    me = y * NGRP + g
    table = block_table.reshape(NGRP, 2, NSEQ, 32).transpose(2, 0, 1, 3).reshape(NDEV, 64)
    spot = jnp.arange(64, dtype=jnp.int32)[None]
    code = (table % 64) * 64 + spot
    mine = table // 64 == me
    low = jnp.min(jnp.where(mine, code, 1 << 20), axis=1)
    high = jnp.max(jnp.where(mine, code, -1), axis=1)
    codes = jnp.stack([low, high], axis=1)
    slots = codes // 64
    second = codes % 64 // 32
    column = (jnp.arange(NDEV, dtype=jnp.int32) // NGRP)[:, None] * 32 + codes % 32
    pairs = jnp.tile(lengths.reshape(NGRP, 2), (NSEQ, 1))
    length = jnp.where(second == 0, pairs[:, :1], pairs[:, 1:])
    limit = jnp.clip(length - column * BLK, 0, BLK)
    idx = jnp.concatenate([
        slots.reshape(-1),
        jnp.where(second == 0, limit, 0).reshape(-1),
        jnp.where(second == 1, limit, 0).reshape(-1),
    ])
    chosen = slots.reshape(-1)[:, None] == jnp.arange(64, dtype=jnp.int32)[None]
    scales = block_scale.reshape(64, 2).astype(jnp.float32)
    scal = jnp.sum(jnp.where(chosen[None], scales.T[:, None, :], 0.0), axis=2).reshape(-1)
    own = lax.dynamic_slice(block_table, (2 * g, 32 * y), (2, 32)).reshape(64)
    before = (own[None, :] // 64 == own[:, None] // 64) & (own[None, :] < own[:, None])
    place = (own // 64) * 2 + jnp.sum(before.astype(jnp.int32), axis=1)

    vmem = pl.BlockSpec(memory_space=pltpu.VMEM)
    smem = pl.BlockSpec(memory_space=pltpu.SMEM)
    hbm = pl.BlockSpec(memory_space=pl.ANY)
    dma = pltpu.SemaphoreType.DMA
    arrived, summed, decode_scale = pl.pallas_call(
        exchange_kernel,
        out_shape=(
            jax.ShapeDtypeStruct((NDEV, 512, BLK), jnp.bfloat16),
            jax.ShapeDtypeStruct((2, 256), jnp.bfloat16),
            jax.ShapeDtypeStruct((64, 2), jnp.bfloat16),
        ),
        in_specs=[smem, smem, hbm, vmem, hbm, vmem],
        out_specs=(vmem, vmem, vmem),
        scratch_shapes=[
            pltpu.VMEM((64, BLK, BLK), jnp.bfloat16),
            pltpu.VMEM((64, BLK, BLK), jnp.bfloat16),
            pltpu.VMEM((NDEV, 512, BLK), jnp.bfloat16),
            pltpu.VMEM((NGRP, 16, BLK), jnp.bfloat16),
            pltpu.VMEM((1024, 256), jnp.bfloat16),
            pltpu.VMEM((NDEV, 8, BLK), jnp.float32),
            pltpu.VMEM((NDEV, 8, BLK), jnp.float32),
            pltpu.VMEM((4, BLK), jnp.float32),
            pltpu.VMEM((NDEV, 4, BLK), jnp.float32),
            pltpu.VMEM((NTP, 2, 256), jnp.float32),
            pltpu.VMEM((NTP, 2, 256), jnp.float32),
            dma((2,)), dma, dma((NGRP,)), dma((NGRP,)),
            dma((4, NDEV)), dma((4, NDEV)),
            dma((NDEV,)), dma((NDEV,)), dma((NDEV,)), dma((NDEV,)),
            dma((NTP,)), dma((NTP,)),
        ],
        compiler_params=pltpu.CompilerParams(collective_id=0, has_side_effects=True),
    )(
        idx, scal, cache_pool.reshape(64, 256, BLK), queries.reshape(16, BLK), output_weight, place[:, None],
    )
    decode_cache = pl.pallas_call(
        place_kernel,
        out_shape=jax.ShapeDtypeStruct((64, 256, BLK), jnp.bfloat16),
        in_specs=[smem, vmem],
        out_specs=hbm,
        scratch_shapes=[dma],
    )(place, arrived.reshape(64, 256, BLK))
    return (
        summed,
        decode_cache.reshape(2, 32, 1, 2, BLK, BLK),
        decode_scale.reshape(2, 32, 1, 2),
    )


def solution(mesh):
    placed = (
        P("grp", "tp", None),
        P(("seq", "grp"), "tp", None, None, None),
        P(("seq", "grp"), "tp", None),
        P(),
        P(),
        P("tp", ("seq", "grp")),
    )
    return jax.shard_map(
        per_device,
        mesh=mesh,
        in_specs=placed,
        out_specs=(
            P("tp", ("seq", "grp")),
            P("grp", "seq", "tp", None, None, None),
            P("grp", "seq", "tp", None),
        ),
        check_vma=False,
    )
```

```python
import functools
import math

import jax
import jax.numpy as jnp
from jax import lax
from jax.experimental import pallas as pl
from jax.experimental.pallas import tpu as pltpu
from jax.sharding import PartitionSpec as P

MESH = pl.DeviceIdType.MESH
ABSENT = -1e30
NSEQ, NTP, NGRP = 4, 8, 8
NDEV = NSEQ * NGRP
BLK = 128
ROOT = 1.0 / math.sqrt(128.0)
START = (0, 256, 128, 384)


def spread(i):
    turn, rest = i // 8, i % 8
    dy, dc = rest // 2, rest % 2
    return dy, (dy + turn) % 4, dc


def exchange_kernel(
    table_hbm, lengths_hbm, scale_hbm, pool_hbm, q_hbm, w_hbm,
    arr, out_ref, scale_out, place_out,
    table, scale_in, codes_v, scales_v, codes, scal, lens,
    pool_k, pool_v, send, q_ref, qall, w, pmsg, part, amsg, att, pout, zbuf,
    in_sem, q_ssem, q_rsem, b_ssem, b_rsem, p_ssem, p_rsem, a_ssem, a_rsem, z_ssem, z_rsem,
):
    y = lax.axis_index("seq")
    z = lax.axis_index("tp")
    g = lax.axis_index("grp")
    me = y * NGRP + g

    def peer(i):
        dy, dx, dc = spread(i)
        ty = (y + dy) % 4
        tg = ((g // 2 + dx) % 4) * 2 + (g + dc) % 2
        return ty, tg

    table_in = pltpu.make_async_copy(table_hbm, table, in_sem.at[0])
    keys_in = pltpu.make_async_copy(pool_hbm.at[:, pl.ds(0, BLK)], pool_k, in_sem.at[1])
    vals_in = pltpu.make_async_copy(pool_hbm.at[:, pl.ds(BLK, BLK)], pool_v, in_sem.at[2])
    q_in = pltpu.make_async_copy(q_hbm, q_ref, in_sem.at[3])
    scales_in = pltpu.make_async_copy(scale_hbm, scale_in, in_sem.at[4])
    lens_in = pltpu.make_async_copy(lengths_hbm, lens, in_sem.at[5])
    w_in = pltpu.make_async_copy(w_hbm, w, in_sem.at[6])
    codes_out = pltpu.make_async_copy(codes_v, codes, in_sem.at[7])
    scales_out = pltpu.make_async_copy(scales_v, scal, in_sem.at[8])
    for copy in (table_in, q_in, keys_in, scales_in, lens_in, vals_in, w_in):
        copy.start()

    barrier = pltpu.get_barrier_semaphore()

    def greet(i, carry):
        ty, tg = peer(i)
        pl.semaphore_signal(barrier, inc=1, device_id={"seq": ty, "grp": tg}, device_id_type=MESH)
        return carry

    lax.fori_loop(1, NDEV, greet, 0)

    def greet_z(i, carry):
        pl.semaphore_signal(barrier, inc=1, device_id={"tp": (z + i) % NTP}, device_id_type=MESH)
        return carry

    lax.fori_loop(1, NTP, greet_z, 0)

    row16 = lax.broadcasted_iota(jnp.int32, (16, BLK), 0)
    lane16 = lax.broadcasted_iota(jnp.int32, (16, BLK), 1)
    table_in.wait()
    names = table[...]
    code = (names & 63) * 64 + (row16 & 1) * 32 + (lane16 & 31)
    mine = (names >> 6) == me
    low = jnp.where(mine, code, 8191)
    high = jnp.where(mine, code, -1)
    found = jnp.zeros((16, BLK), jnp.int32)
    for qq in range(NSEQ):
        part_of = (lane16 >> 5) == qq
        least = jnp.min(jnp.where(part_of, low, 8191), axis=1, keepdims=True)
        most = jnp.max(jnp.where(part_of, high, -1), axis=1, keepdims=True)
        found = jnp.where(lane16 == qq, least, jnp.where(lane16 == 4 + qq, most, found))
    other = pltpu.roll(found, 15, 0)
    codes_v[...] = jnp.where(lane16 < 4, jnp.minimum(found, other), jnp.maximum(found, other))
    codes_out.start()
    q_in.wait()
    qall[g] = q_ref[...]
    scales_in.wait()
    scales_v[...] = scale_in[...].astype(jnp.float32)
    scales_out.start()
    codes_out.wait()

    def code_of(q, gg, r):
        return codes[2 * gg, q + 4 * r]

    def pick(c):
        pool, r = (pool_k, pool_v)[c // 2], c % 2

        def body(t, carry):
            slot = (code_of(t // NGRP, t % NGRP, r) >> 6) & 63
            send[t, pl.ds(START[c], BLK), :] = pool[slot]
            return carry

        lax.fori_loop(0, NDEV, body, 0)

    def block_copy(c, i):
        ty, tg = peer(i)
        rows = pl.ds(START[c], BLK)
        return pltpu.make_async_remote_copy(
            src_ref=send.at[ty * NGRP + tg, rows],
            dst_ref=arr.at[me, rows],
            send_sem=b_ssem.at[c, i],
            recv_sem=b_rsem.at[c, i],
            device_id={"seq": ty, "grp": tg},
            device_id_type=MESH,
        )

    def send_wave(c):
        def body(i, carry):
            block_copy(c, i).start()
            return carry

        lax.fori_loop(1, NDEV, body, 0)

    def q_copy(i):
        tg = (g + i) % NGRP
        return pltpu.make_async_remote_copy(
            src_ref=q_ref, dst_ref=qall.at[g], send_sem=q_ssem.at[i], recv_sem=q_rsem.at[i],
            device_id={"grp": tg}, device_id_type=MESH,
        )

    keys_in.wait()
    pick(0)
    pl.semaphore_wait(barrier, NDEV - 1 + NTP - 1)
    for i in range(1, NGRP):
        q_copy(i).start()
    send_wave(0)
    pick(1)
    vals_in.wait()
    pick(2)
    pick(3)
    scales_out.wait()
    lens_in.wait()
    for i in range(1, NGRP):
        q_copy(i).wait()

    row4 = lax.broadcasted_iota(jnp.int32, (4, BLK), 0)
    lane4 = lax.broadcasted_iota(jnp.int32, (4, BLK), 1)

    def attend(gg, carry):
        q = qall[gg]
        scores, masks, key_scales, value_scales = [], [], [], []
        for n in range(8):
            t, r = (n // 2) * NGRP + gg, n % 2
            found_at = code_of(n // 2, gg, r)
            slot, row, column = (found_at >> 6) & 63, (found_at >> 5) & 1, (n // 2) * 32 + (found_at & 31)
            keys = send[t, pl.ds(r * 256, BLK), :]
            s = lax.dot_general(q, keys, (((1,), (1,)), ((), ())), preferred_element_type=jnp.float32)
            s = s * (scal[0, slot] * ROOT)
            value_scales.append(scal[1, slot])
            key_scales.append(scal[0, slot])
            limit = jnp.where((row16 >> 3) == row, lens[2 * gg + row] - column * BLK, 0)
            live = lane16 < limit
            scores.append(jnp.where(live, s, ABSENT))
            masks.append(live)
        top = functools.reduce(jnp.maximum, scores)
        peak = jnp.max(top, axis=1, keepdims=True)
        total = jnp.zeros((16, BLK), jnp.float32)
        acc = jnp.zeros((16, BLK), jnp.float32)
        for n in range(8):
            t, r = (n // 2) * NGRP + gg, n % 2
            weight = jnp.where(masks[n], jnp.exp(scores[n] - peak), 0.0)
            total = total + weight
            scaled = (weight * value_scales[n]).astype(jnp.bfloat16)
            acc = acc + jnp.dot(scaled, send[t, pl.ds(r * 256 + BLK, BLK), :], preferred_element_type=jnp.float32)
        denom = jnp.sum(total, axis=1, keepdims=True)
        stats = jnp.where(lane16 == 2, peak, jnp.where(lane16 == 3, denom, 0.0))
        for qq in range(NSEQ):
            t = qq * NGRP + gg
            pmsg[t, pl.ds(0, 4), :] = acc[4 * qq : 4 * qq + 4]
            low = stats[4 * qq : 4 * qq + 4]
            for r in range(2):
                low = jnp.where((row4 == r) & (lane4 == 0), key_scales[2 * qq + r], low)
                low = jnp.where((row4 == r) & (lane4 == 1), value_scales[2 * qq + r], low)
            pmsg[t, pl.ds(4, 4), :] = low
        return carry

    lax.fori_loop(0, NGRP, attend, 0)

    def p_copy(i):
        ty, tg = peer(i)
        return pltpu.make_async_remote_copy(
            src_ref=pmsg.at[ty * NGRP + tg], dst_ref=part.at[me],
            send_sem=p_ssem.at[i], recv_sem=p_rsem.at[i],
            device_id={"seq": ty, "grp": tg}, device_id_type=MESH,
        )

    def a_copy(i):
        ty, tg = peer(i)
        return pltpu.make_async_remote_copy(
            src_ref=amsg, dst_ref=att.at[(y % 2) * 16 + g * 2 + y // 2],
            send_sem=a_ssem.at[i], recv_sem=a_rsem.at[i],
            device_id={"seq": ty, "grp": tg}, device_id_type=MESH,
        )

    def each(make, what, first, last):
        def body(i, carry):
            getattr(make(i), what)()
            return carry

        lax.fori_loop(first, last, body, 0)

    each(p_copy, "start", 1, NDEV)
    part[me] = pmsg[me]
    send_wave(1)
    each(p_copy, "wait", 1, NDEV)

    peaks = part[:, pl.ds(4, 4), 2:3]
    sums = part[:, pl.ds(4, 4), 3:4]
    peak = jnp.max(peaks, axis=0, keepdims=True)
    factor = jnp.exp(peaks - peak)
    denom = jnp.sum(sums * factor, axis=0)
    numer = jnp.sum(part[:, pl.ds(0, 4), :] * factor, axis=0)
    rows = (numer / denom).astype(jnp.bfloat16).astype(jnp.float32)
    amsg[...] = rows
    att[(y % 2) * 16 + g * 2 + y // 2] = rows
    each(a_copy, "start", 1, NDEV)
    send_wave(2)
    send_wave(3)
    arr[me] = send[me]
    wide = lax.broadcasted_iota(jnp.int32, (8, BLK), 1)
    first = pltpu.roll(jnp.broadcast_to(table[pl.ds(2 * g, 1), :], (8, BLK)), (BLK - 32 * y) % BLK, 1)
    second = pltpu.roll(jnp.broadcast_to(table[pl.ds(2 * g + 1, 1), :], (8, BLK)), (BLK + 32 - 32 * y) % BLK, 1)
    own = jnp.where(wide < 32, first, second)[0:1]
    across = jnp.broadcast_to(own, (BLK, BLK))
    down = across.T
    inside = lax.broadcasted_iota(jnp.int32, (BLK, BLK), 0) < 64
    before = inside & ((down >> 6) == (across >> 6)) & (down < across)
    rank = jnp.sum(before.astype(jnp.int32), axis=0, keepdims=True)
    place_out[...] = ((own >> 6) * 2 + rank) & 63
    lines = lax.broadcasted_iota(jnp.int32, (256, BLK), 0)
    hot = (lines == (own >> 6) * 8 + 4 + rank).astype(jnp.float32).astype(jnp.bfloat16)
    flat = part[...].reshape(256, BLK).T[0:8].astype(jnp.bfloat16)
    picked = jnp.dot(flat, hot, preferred_element_type=jnp.float32).astype(jnp.bfloat16)
    scale_out[0] = picked[0:2, 0:32]
    scale_out[1] = picked[0:2, 32:64]
    w_in.wait()
    each(a_copy, "wait", 1, NDEV)

    total = jnp.zeros((16, 256), jnp.float32)
    for h in range(8):
        lhs = att[pl.ds((h // 4) * 16, 16), h % 4, :].astype(jnp.bfloat16)
        total = total + jnp.dot(lhs, w[pl.ds(h * BLK, BLK), :], preferred_element_type=jnp.float32)
    for k in range(NTP):
        pout[k] = total[2 * k : 2 * k + 2]

    def z_copy(i):
        tz = (z + i) % NTP
        return pltpu.make_async_remote_copy(
            src_ref=pout.at[tz], dst_ref=zbuf.at[z], send_sem=z_ssem.at[i], recv_sem=z_rsem.at[i],
            device_id={"tp": tz}, device_id_type=MESH,
        )

    each(z_copy, "start", 1, NTP)
    zbuf[z] = pout[z]
    each(z_copy, "wait", 1, NTP)
    out_ref[...] = jnp.sum(zbuf[...], axis=0).astype(jnp.bfloat16)

    for c in range(4):
        each(functools.partial(block_copy, c), "wait", 1, NDEV)


def place_kernel(src, arr, summed, scales, out, out_sum, out_scales, sem):
    small = (
        pltpu.make_async_copy(summed, out_sum, sem.at[1]),
        pltpu.make_async_copy(scales, out_scales, sem.at[2]),
    )
    for copy in small:
        copy.start()

    def put(p, carry):
        pltpu.make_async_copy(arr.at[src[0, p]], out.at[p], sem.at[0]).start()
        return carry

    lax.fori_loop(0, 64, put, 0, unroll=8)
    for copy in small:
        copy.wait()
    pltpu.make_async_copy(arr, out, sem.at[0]).wait()


def per_device(queries, cache_pool, block_scale, block_table, lengths, output_weight):
    vmem = pl.BlockSpec(memory_space=pltpu.VMEM)
    smem = pl.BlockSpec(memory_space=pltpu.SMEM)
    hbm = pl.BlockSpec(memory_space=pltpu.HBM)
    anywhere = pl.BlockSpec(memory_space=pl.ANY)
    dma = pltpu.SemaphoreType.DMA
    arrived, summed, scales, place = pl.pallas_call(
        exchange_kernel,
        out_shape=(
            jax.ShapeDtypeStruct((NDEV, 512, BLK), jnp.bfloat16),
            jax.ShapeDtypeStruct((2, 256), jnp.bfloat16),
            jax.ShapeDtypeStruct((2, 2, 32), jnp.bfloat16),
            jax.ShapeDtypeStruct((1, BLK), jnp.int32),
        ),
        in_specs=[hbm] * 6,
        out_specs=(vmem, vmem, vmem, vmem),
        scratch_shapes=[
            pltpu.VMEM((16, BLK), jnp.int32),
            pltpu.VMEM((2, 64), jnp.bfloat16),
            pltpu.VMEM((16, BLK), jnp.int32),
            pltpu.VMEM((2, 64), jnp.float32),
            pltpu.SMEM((16, BLK), jnp.int32),
            pltpu.SMEM((2, 64), jnp.float32),
            pltpu.SMEM((16,), jnp.int32),
            pltpu.VMEM((64, BLK, BLK), jnp.bfloat16),
            pltpu.VMEM((64, BLK, BLK), jnp.bfloat16),
            pltpu.VMEM((NDEV, 512, BLK), jnp.bfloat16),
            pltpu.VMEM((16, BLK), jnp.bfloat16),
            pltpu.VMEM((NGRP, 16, BLK), jnp.bfloat16),
            pltpu.VMEM((1024, 256), jnp.bfloat16),
            pltpu.VMEM((NDEV, 8, BLK), jnp.float32),
            pltpu.VMEM((NDEV, 8, BLK), jnp.float32),
            pltpu.VMEM((4, BLK), jnp.float32),
            pltpu.VMEM((NDEV, 4, BLK), jnp.float32),
            pltpu.VMEM((NTP, 2, 256), jnp.float32),
            pltpu.VMEM((NTP, 2, 256), jnp.float32),
            dma((9,)), dma((NGRP,)), dma((NGRP,)),
            dma((4, NDEV)), dma((4, NDEV)),
            dma((NDEV,)), dma((NDEV,)), dma((NDEV,)), dma((NDEV,)),
            dma((NTP,)), dma((NTP,)),
        ],
        compiler_params=pltpu.CompilerParams(
            collective_id=0, has_side_effects=True, vmem_limit_bytes=24 << 20
        ),
    )(*(
        pltpu.with_memory_space_constraint(operand, pltpu.HBM)
        for operand in (
            block_table, lengths, block_scale.reshape(64, 2).T, cache_pool.reshape(64, 256, BLK),
            queries.reshape(16, BLK), output_weight,
        )
    ))
    decode_cache, attention_output, decode_scale = pl.pallas_call(
        place_kernel,
        out_shape=(
            jax.ShapeDtypeStruct((64, 256, BLK), jnp.bfloat16),
            jax.ShapeDtypeStruct((2, 256), jnp.bfloat16),
            jax.ShapeDtypeStruct((2, 2, 32), jnp.bfloat16),
        ),
        in_specs=[smem, vmem, vmem, vmem],
        out_specs=(hbm, hbm, hbm),
        scratch_shapes=[dma((3,))],
        compiler_params=pltpu.CompilerParams(vmem_limit_bytes=12 << 20),
    )(place, arrived.reshape(64, 256, BLK), summed, scales)
    return (
        attention_output,
        decode_cache.reshape(2, 32, 1, 2, BLK, BLK),
        decode_scale.transpose(0, 2, 1).reshape(2, 32, 1, 2),
    )


def solution(mesh):
    placed = (
        P("grp", "tp", None),
        P(("seq", "grp"), "tp", None, None, None),
        P(("seq", "grp"), "tp", None),
        P(),
        P(),
        P("tp", ("seq", "grp")),
    )
    return jax.shard_map(
        per_device,
        mesh=mesh,
        in_specs=placed,
        out_specs=(
            P("tp", ("seq", "grp")),
            P("grp", "seq", "tp", None, None, None),
            P("grp", "seq", "tp", None),
        ),
        check_vma=False,
    )
```

```python
import functools
import math

import jax
import jax.numpy as jnp
from jax import lax
from jax.experimental import pallas as pl
from jax.experimental.pallas import tpu as pltpu
from jax.sharding import PartitionSpec as P

MESH = pl.DeviceIdType.MESH
ABSENT = -1e30
NSEQ, NTP, NGRP = 4, 8, 8
NDEV = NSEQ * NGRP
BLK = 128
ROOT = 1.0 / math.sqrt(128.0)
START = (0, 256, 128, 384)


PEERS = [
    (dy, (dy + turn) % 4, dc)
    for turn in range(4) for dy in range(4) for dc in range(2)
    if (dy, turn, dc) != (0, 0, 0)
]


def exchange_kernel(
    table_hbm, lengths_hbm, scale_hbm, pool_hbm, q_hbm, w_hbm,
    arr, out_ref, scale_out, place_out,
    table, scale_in, codes_v, scales_v, codes, scal, lens,
    pool_k, pool_v, send, q_ref, qall, w, pmsg, part, amsg, att, pout, zbuf,
    in_sem, q_sem, b_sem, p_sem, a_sem, z_sem,
):
    y = lax.axis_index("seq")
    z = lax.axis_index("tp")
    g = lax.axis_index("grp")
    me = y * NGRP + g

    ys = [(y + k) % NSEQ for k in range(NSEQ)]
    xs = [((g // 2 + k) % 4) * 2 for k in range(4)]
    cs = [(g + k) % 2 for k in range(2)]

    def peer(offset):
        dy, dx, dc = offset
        return ys[dy], xs[dx] + cs[dc]

    table_in = pltpu.make_async_copy(table_hbm, table, in_sem.at[0])
    keys_in = pltpu.make_async_copy(pool_hbm.at[:, pl.ds(0, BLK)], pool_k, in_sem.at[1])
    vals_in = pltpu.make_async_copy(pool_hbm.at[:, pl.ds(BLK, BLK)], pool_v, in_sem.at[2])
    q_in = pltpu.make_async_copy(q_hbm, q_ref, in_sem.at[3])
    scales_in = pltpu.make_async_copy(scale_hbm, scale_in, in_sem.at[4])
    lens_in = pltpu.make_async_copy(lengths_hbm, lens, in_sem.at[5])
    w_in = pltpu.make_async_copy(w_hbm, w, in_sem.at[6])
    codes_out = pltpu.make_async_copy(codes_v, codes, in_sem.at[7])
    scales_out = pltpu.make_async_copy(scales_v, scal, in_sem.at[8])
    for copy in (table_in, q_in, keys_in, scales_in, lens_in, vals_in, w_in):
        copy.start()

    barrier = pltpu.get_barrier_semaphore()
    for offset in PEERS:
        ty, tg = peer(offset)
        pl.semaphore_signal(barrier, inc=1, device_id={"seq": ty, "grp": tg}, device_id_type=MESH)
    for k in range(1, NTP):
        pl.semaphore_signal(barrier, inc=1, device_id={"tp": (z + k) % NTP}, device_id_type=MESH)

    row16 = lax.broadcasted_iota(jnp.int32, (16, BLK), 0)
    lane16 = lax.broadcasted_iota(jnp.int32, (16, BLK), 1)
    table_in.wait()
    names = table[...]
    code = (names & 63) * 64 + (row16 & 1) * 32 + (lane16 & 31)
    mine = (names >> 6) == me
    low = jnp.where(mine, code, 8191)
    high = jnp.where(mine, code, -1)
    found = jnp.zeros((16, BLK), jnp.int32)
    for qq in range(NSEQ):
        part_of = (lane16 >> 5) == qq
        least = jnp.min(jnp.where(part_of, low, 8191), axis=1, keepdims=True)
        most = jnp.max(jnp.where(part_of, high, -1), axis=1, keepdims=True)
        found = jnp.where(lane16 == qq, least, jnp.where(lane16 == 4 + qq, most, found))
    other = pltpu.roll(found, 15, 0)
    codes_v[...] = jnp.where(lane16 < 4, jnp.minimum(found, other), jnp.maximum(found, other))
    codes_out.start()
    q_in.wait()
    qall[g] = q_ref[...]
    scales_in.wait()
    scales_v[...] = scale_in[...].astype(jnp.float32)
    scales_out.start()
    codes_out.wait()

    def code_of(q, gg, r):
        return codes[2 * gg, q + 4 * r]

    def pick(c):
        pool, r = (pool_k, pool_v)[c // 2], c % 2

        def body(t, carry):
            slot = (code_of(t // NGRP, t % NGRP, r) >> 6) & 63
            send[t, pl.ds(START[c], BLK), :] = pool[slot]
            return carry

        lax.fori_loop(0, NDEV, body, 0)

    def remote(src, dst, sems, device):
        return pltpu.make_async_remote_copy(
            src_ref=src, dst_ref=dst, send_sem=sems.at[0], recv_sem=sems.at[1],
            device_id=device, device_id_type=MESH,
        )

    def send_wave(c):
        rows = pl.ds(START[c], BLK)
        for offset in PEERS:
            ty, tg = peer(offset)
            remote(send.at[ty * NGRP + tg, rows], arr.at[me, rows], b_sem, {"seq": ty, "grp": tg}).start()

    here = {"seq": ys[1]}
    rest = pl.ds(0, NDEV - 1)
    q_all = remote(qall.at[pl.ds(0, NGRP - 1)], qall.at[pl.ds(0, NGRP - 1)], q_sem, here)
    b_all = remote(send.at[rest], arr.at[rest], b_sem, here)
    p_all = remote(pmsg.at[rest], part.at[rest], p_sem, here)
    a_all = remote(att.at[rest], att.at[rest], a_sem, here)
    z_all = remote(pout.at[pl.ds(0, NTP - 1)], zbuf.at[pl.ds(0, NTP - 1)], z_sem, here)

    keys_in.wait()
    pick(0)
    pl.semaphore_wait(barrier, NDEV - 1 + NTP - 1)
    for k in range(1, NGRP):
        remote(q_ref, qall.at[g], q_sem, {"grp": (g + k) % NGRP}).start()
    send_wave(0)
    pick(1)
    vals_in.wait()
    pick(2)
    pick(3)
    scales_out.wait()
    lens_in.wait()
    q_all.wait_recv()

    row4 = lax.broadcasted_iota(jnp.int32, (4, BLK), 0)
    lane4 = lax.broadcasted_iota(jnp.int32, (4, BLK), 1)

    def attend(gg, carry):
        q = qall[gg]
        scores, masks, key_scales, value_scales = [], [], [], []
        for n in range(8):
            t, r = (n // 2) * NGRP + gg, n % 2
            found_at = code_of(n // 2, gg, r)
            slot, row, column = (found_at >> 6) & 63, (found_at >> 5) & 1, (n // 2) * 32 + (found_at & 31)
            keys = send[t, pl.ds(r * 256, BLK), :]
            s = lax.dot_general(q, keys, (((1,), (1,)), ((), ())), preferred_element_type=jnp.float32)
            s = s * (scal[0, slot] * ROOT)
            value_scales.append(scal[1, slot])
            key_scales.append(scal[0, slot])
            limit = jnp.where((row16 >> 3) == row, lens[2 * gg + row] - column * BLK, 0)
            live = lane16 < limit
            scores.append(jnp.where(live, s, ABSENT))
            masks.append(live)
        top = functools.reduce(jnp.maximum, scores)
        peak = jnp.max(top, axis=1, keepdims=True)
        total = jnp.zeros((16, BLK), jnp.float32)
        acc = jnp.zeros((16, BLK), jnp.float32)
        for n in range(8):
            t, r = (n // 2) * NGRP + gg, n % 2
            weight = jnp.where(masks[n], jnp.exp(scores[n] - peak), 0.0)
            total = total + weight
            scaled = (weight * value_scales[n]).astype(jnp.bfloat16)
            acc = acc + jnp.dot(scaled, send[t, pl.ds(r * 256 + BLK, BLK), :], preferred_element_type=jnp.float32)
        denom = jnp.sum(total, axis=1, keepdims=True)
        stats = jnp.where(lane16 == 2, peak, jnp.where(lane16 == 3, denom, 0.0))
        for qq in range(NSEQ):
            t = qq * NGRP + gg
            pmsg[t, pl.ds(0, 4), :] = acc[4 * qq : 4 * qq + 4]
            low = stats[4 * qq : 4 * qq + 4]
            for r in range(2):
                low = jnp.where((row4 == r) & (lane4 == 0), key_scales[2 * qq + r], low)
                low = jnp.where((row4 == r) & (lane4 == 1), value_scales[2 * qq + r], low)
            pmsg[t, pl.ds(4, 4), :] = low
        return carry

    lax.fori_loop(0, NGRP, attend, 0)

    for offset in PEERS:
        ty, tg = peer(offset)
        remote(pmsg.at[ty * NGRP + tg], part.at[me], p_sem, {"seq": ty, "grp": tg}).start()
    part[me] = pmsg[me]
    send_wave(1)
    p_all.wait_recv()

    peaks = part[:, pl.ds(4, 4), 2:3]
    sums = part[:, pl.ds(4, 4), 3:4]
    peak = jnp.max(peaks, axis=0, keepdims=True)
    factor = jnp.exp(peaks - peak)
    denom = jnp.sum(sums * factor, axis=0)
    numer = jnp.sum(part[:, pl.ds(0, 4), :] * factor, axis=0)
    rows = (numer / denom).astype(jnp.bfloat16).astype(jnp.float32)
    amsg[...] = rows
    att[(y % 2) * 16 + g * 2 + y // 2] = rows
    for offset in PEERS:
        ty, tg = peer(offset)
        remote(amsg, att.at[(y % 2) * 16 + g * 2 + y // 2], a_sem, {"seq": ty, "grp": tg}).start()
    send_wave(2)
    send_wave(3)
    arr[me] = send[me]
    wide = lax.broadcasted_iota(jnp.int32, (8, BLK), 1)
    first = pltpu.roll(jnp.broadcast_to(table[pl.ds(2 * g, 1), :], (8, BLK)), (BLK - 32 * y) % BLK, 1)
    second = pltpu.roll(jnp.broadcast_to(table[pl.ds(2 * g + 1, 1), :], (8, BLK)), (BLK + 32 - 32 * y) % BLK, 1)
    own = jnp.where(wide < 32, first, second)[0:1]
    across = jnp.broadcast_to(own, (BLK, BLK))
    down = across.T
    inside = lax.broadcasted_iota(jnp.int32, (BLK, BLK), 0) < 64
    before = inside & ((down >> 6) == (across >> 6)) & (down < across)
    rank = jnp.sum(before.astype(jnp.int32), axis=0, keepdims=True)
    place_out[...] = ((own >> 6) * 2 + rank) & 63
    lines = lax.broadcasted_iota(jnp.int32, (256, BLK), 0)
    hot = (lines == (own >> 6) * 8 + 4 + rank).astype(jnp.float32).astype(jnp.bfloat16)
    flat = part[...].reshape(256, BLK).T[0:8].astype(jnp.bfloat16)
    picked = jnp.dot(flat, hot, preferred_element_type=jnp.float32).astype(jnp.bfloat16)
    scale_out[0] = picked[0:2, 0:32]
    scale_out[1] = picked[0:2, 32:64]
    w_in.wait()
    a_all.wait_recv()

    total = jnp.zeros((16, 256), jnp.float32)
    for h in range(8):
        lhs = att[pl.ds((h // 4) * 16, 16), h % 4, :].astype(jnp.bfloat16)
        total = total + jnp.dot(lhs, w[pl.ds(h * BLK, BLK), :], preferred_element_type=jnp.float32)
    for k in range(NTP):
        pout[k] = total[2 * k : 2 * k + 2]

    for k in range(1, NTP):
        tz = (z + k) % NTP
        remote(pout.at[tz], zbuf.at[z], z_sem, {"tp": tz}).start()
    zbuf[z] = pout[z]
    z_all.wait_recv()
    out_ref[...] = jnp.sum(zbuf[...], axis=0).astype(jnp.bfloat16)

    for phase in (q_all, p_all, a_all, z_all, b_all):
        phase.wait_send()
    b_all.wait_recv()


def place_kernel(src, arr, summed, scales, out, out_sum, out_scales, sem):
    small = (
        pltpu.make_async_copy(summed, out_sum, sem.at[1]),
        pltpu.make_async_copy(scales, out_scales, sem.at[2]),
    )
    for copy in small:
        copy.start()

    def put(p, carry):
        pltpu.make_async_copy(arr.at[src[0, p]], out.at[p], sem.at[0]).start()
        return carry

    lax.fori_loop(0, 64, put, 0, unroll=8)
    for copy in small:
        copy.wait()
    pltpu.make_async_copy(arr, out, sem.at[0]).wait()


def per_device(queries, cache_pool, block_scale, block_table, lengths, output_weight):
    vmem = pl.BlockSpec(memory_space=pltpu.VMEM)
    smem = pl.BlockSpec(memory_space=pltpu.SMEM)
    hbm = pl.BlockSpec(memory_space=pltpu.HBM)
    anywhere = pl.BlockSpec(memory_space=pl.ANY)
    dma = pltpu.SemaphoreType.DMA
    arrived, summed, scales, place = pl.pallas_call(
        exchange_kernel,
        out_shape=(
            jax.ShapeDtypeStruct((NDEV, 512, BLK), jnp.bfloat16),
            jax.ShapeDtypeStruct((2, 256), jnp.bfloat16),
            jax.ShapeDtypeStruct((2, 2, 32), jnp.bfloat16),
            jax.ShapeDtypeStruct((1, BLK), jnp.int32),
        ),
        in_specs=[hbm] * 6,
        out_specs=(vmem, vmem, vmem, vmem),
        scratch_shapes=[
            pltpu.VMEM((16, BLK), jnp.int32),
            pltpu.VMEM((2, 64), jnp.bfloat16),
            pltpu.VMEM((16, BLK), jnp.int32),
            pltpu.VMEM((2, 64), jnp.float32),
            pltpu.SMEM((16, BLK), jnp.int32),
            pltpu.SMEM((2, 64), jnp.float32),
            pltpu.SMEM((16,), jnp.int32),
            pltpu.VMEM((64, BLK, BLK), jnp.bfloat16),
            pltpu.VMEM((64, BLK, BLK), jnp.bfloat16),
            pltpu.VMEM((NDEV, 512, BLK), jnp.bfloat16),
            pltpu.VMEM((16, BLK), jnp.bfloat16),
            pltpu.VMEM((NGRP, 16, BLK), jnp.bfloat16),
            pltpu.VMEM((1024, 256), jnp.bfloat16),
            pltpu.VMEM((NDEV, 8, BLK), jnp.float32),
            pltpu.VMEM((NDEV, 8, BLK), jnp.float32),
            pltpu.VMEM((4, BLK), jnp.float32),
            pltpu.VMEM((NDEV, 4, BLK), jnp.float32),
            pltpu.VMEM((NTP, 2, 256), jnp.float32),
            pltpu.VMEM((NTP, 2, 256), jnp.float32),
            dma((9,)), dma((2,)), dma((2,)), dma((2,)), dma((2,)), dma((2,)),
        ],
        compiler_params=pltpu.CompilerParams(
            collective_id=0, has_side_effects=True, vmem_limit_bytes=24 << 20
        ),
    )(*(
        pltpu.with_memory_space_constraint(operand, pltpu.HBM)
        for operand in (
            block_table, lengths, block_scale.reshape(64, 2).T, cache_pool.reshape(64, 256, BLK),
            queries.reshape(16, BLK), output_weight,
        )
    ))
    decode_cache, attention_output, decode_scale = pl.pallas_call(
        place_kernel,
        out_shape=(
            jax.ShapeDtypeStruct((64, 256, BLK), jnp.bfloat16),
            jax.ShapeDtypeStruct((2, 256), jnp.bfloat16),
            jax.ShapeDtypeStruct((2, 2, 32), jnp.bfloat16),
        ),
        in_specs=[smem, vmem, vmem, vmem],
        out_specs=(hbm, hbm, hbm),
        scratch_shapes=[dma((3,))],
        compiler_params=pltpu.CompilerParams(vmem_limit_bytes=12 << 20),
    )(place, arrived.reshape(64, 256, BLK), summed, scales)
    return (
        attention_output,
        decode_cache.reshape(2, 32, 1, 2, BLK, BLK),
        decode_scale.transpose(0, 2, 1).reshape(2, 32, 1, 2),
    )


def solution(mesh):
    placed = (
        P("grp", "tp", None),
        P(("seq", "grp"), "tp", None, None, None),
        P(("seq", "grp"), "tp", None),
        P(),
        P(),
        P("tp", ("seq", "grp")),
    )
    return jax.shard_map(
        per_device,
        mesh=mesh,
        in_specs=placed,
        out_specs=(
            P("tp", ("seq", "grp")),
            P("grp", "seq", "tp", None, None, None),
            P("grp", "seq", "tp", None),
        ),
        check_vma=False,
    )
```

```python
import functools
import math

import jax
import jax.numpy as jnp
from jax import lax
from jax.experimental import pallas as pl
from jax.experimental.pallas import tpu as pltpu
from jax.sharding import PartitionSpec as P

MESH = pl.DeviceIdType.MESH
ABSENT = -1e30
NSEQ, NTP, NGRP = 4, 8, 8
NDEV = NSEQ * NGRP
BLK = 128
ROOT = 1.0 / math.sqrt(128.0)
START = (0, 256, 128, 384)


PEERS = [
    (dy, (dy + turn) % 4, dc)
    for turn in range(4) for dy in range(4) for dc in range(2)
    if (dy, turn, dc) != (0, 0, 0)
]


def exchange_kernel(
    table_hbm, lengths_hbm, scale_hbm, pool_hbm, q_hbm, w_hbm,
    arr, out_ref, scale_out, place_out,
    table, scale_in, codes_v, scales_v, codes, scal, lens,
    pool_k, pool_v, send, q_ref, qall, w, pmsg, part, smsg, stat, amsg, att, attended, pout, zbuf,
    in_sem, q_sem, b_sem, p_sem, s_sem, a_sem, z_sem,
):
    y = lax.axis_index("seq")
    z = lax.axis_index("tp")
    g = lax.axis_index("grp")
    me = y * NGRP + g

    ys = [(y + k) % NSEQ for k in range(NSEQ)]
    xs = [((g // 2 + k) % 4) * 2 for k in range(4)]
    cs = [(g + k) % 2 for k in range(2)]

    def peer(offset):
        dy, dx, dc = offset
        return ys[dy], xs[dx] + cs[dc]

    table_in = pltpu.make_async_copy(table_hbm, table, in_sem.at[0])
    keys_in = pltpu.make_async_copy(pool_hbm.at[:, pl.ds(0, BLK)], pool_k, in_sem.at[1])
    vals_in = pltpu.make_async_copy(pool_hbm.at[:, pl.ds(BLK, BLK)], pool_v, in_sem.at[2])
    q_in = pltpu.make_async_copy(q_hbm, q_ref, in_sem.at[3])
    scales_in = pltpu.make_async_copy(scale_hbm, scale_in, in_sem.at[4])
    lens_in = pltpu.make_async_copy(lengths_hbm, lens, in_sem.at[5])
    w_in = pltpu.make_async_copy(w_hbm, w, in_sem.at[6])
    codes_out = pltpu.make_async_copy(codes_v, codes, in_sem.at[7])
    scales_out = pltpu.make_async_copy(scales_v, scal, in_sem.at[8])
    for copy in (table_in, q_in, keys_in, scales_in, lens_in, vals_in, w_in):
        copy.start()

    barrier = pltpu.get_barrier_semaphore()
    for offset in PEERS:
        ty, tg = peer(offset)
        pl.semaphore_signal(barrier, inc=1, device_id={"seq": ty, "grp": tg}, device_id_type=MESH)
    for k in range(1, NTP):
        pl.semaphore_signal(barrier, inc=1, device_id={"tp": (z + k) % NTP}, device_id_type=MESH)

    row16 = lax.broadcasted_iota(jnp.int32, (16, BLK), 0)
    lane16 = lax.broadcasted_iota(jnp.int32, (16, BLK), 1)
    table_in.wait()
    names = table[...]
    code = (names & 63) * 64 + (row16 & 1) * 32 + (lane16 & 31)
    mine = (names >> 6) == me
    low = jnp.where(mine, code, 8191)
    high = jnp.where(mine, code, -1)
    found = jnp.zeros((16, BLK), jnp.int32)
    for qq in range(NSEQ):
        part_of = (lane16 >> 5) == qq
        least = jnp.min(jnp.where(part_of, low, 8191), axis=1, keepdims=True)
        most = jnp.max(jnp.where(part_of, high, -1), axis=1, keepdims=True)
        found = jnp.where(lane16 == qq, least, jnp.where(lane16 == 4 + qq, most, found))
    other = pltpu.roll(found, 15, 0)
    codes_v[...] = jnp.where(lane16 < 4, jnp.minimum(found, other), jnp.maximum(found, other))
    codes_out.start()
    q_in.wait()
    qall[g] = q_ref[...]
    scales_in.wait()
    scales_v[...] = scale_in[...].astype(jnp.float32)
    scales_out.start()
    codes_out.wait()

    def code_of(q, gg, r):
        return codes[2 * gg, q + 4 * r]

    def pick_one(c, ty, tg):
        pool, r = (pool_k, pool_v)[c // 2], c % 2
        slot = (code_of(ty, tg, r) >> 6) & 63
        send[ty * NGRP + tg, pl.ds(START[c], BLK), :] = pool[slot]

    def pick(c):
        pool, r = (pool_k, pool_v)[c // 2], c % 2

        def body(t, carry):
            slot = (code_of(t // NGRP, t % NGRP, r) >> 6) & 63
            send[t, pl.ds(START[c], BLK), :] = pool[slot]
            return carry

        lax.fori_loop(0, NDEV, body, 0)

    def remote(src, dst, sems, device):
        return pltpu.make_async_remote_copy(
            src_ref=src, dst_ref=dst, send_sem=sems.at[0], recv_sem=sems.at[1],
            device_id=device, device_id_type=MESH,
        )

    def send_wave(c):
        rows = pl.ds(START[c], BLK)
        for offset in PEERS:
            ty, tg = peer(offset)
            remote(send.at[ty * NGRP + tg, rows], arr.at[me, rows], b_sem, {"seq": ty, "grp": tg}).start()

    here = {"seq": ys[1]}
    rest = pl.ds(0, NDEV - 1)
    q_all = remote(qall.at[pl.ds(0, NGRP - 1)], qall.at[pl.ds(0, NGRP - 1)], q_sem, here)
    b_all = remote(send.at[rest], arr.at[rest], b_sem, here)
    p_all = remote(pmsg.at[rest], part.at[rest], p_sem, here)
    s_all = remote(stat.at[rest], stat.at[rest], s_sem, here)
    a_all = remote(att.at[rest], att.at[rest], a_sem, here)
    z_all = remote(pout.at[pl.ds(0, NTP - 1)], zbuf.at[pl.ds(0, NTP - 1)], z_sem, here)

    keys_in.wait()
    for offset in PEERS:
        pick_one(0, *peer(offset))
    pl.semaphore_wait(barrier, NDEV - 1 + NTP - 1)
    for k in range(1, NGRP):
        remote(q_ref, qall.at[g], q_sem, {"grp": (g + k) % NGRP}).start()
    send_wave(0)
    pick_one(0, y, g)
    pick(1)
    vals_in.wait()
    pick(2)
    pick(3)
    scales_out.wait()
    lens_in.wait()
    q_all.wait_recv()

    lane1 = lax.broadcasted_iota(jnp.int32, (1, BLK), 1)

    def attend(gg, carry):
        q = qall[gg]
        scores, masks, key_scales, value_scales = [], [], [], []
        for n in range(8):
            t, r = (n // 2) * NGRP + gg, n % 2
            found_at = code_of(n // 2, gg, r)
            slot, row, column = (found_at >> 6) & 63, (found_at >> 5) & 1, (n // 2) * 32 + (found_at & 31)
            keys = send[t, pl.ds(r * 256, BLK), :]
            s = lax.dot_general(q, keys, (((1,), (1,)), ((), ())), preferred_element_type=jnp.float32)
            s = s * (scal[0, slot] * ROOT)
            value_scales.append(scal[1, slot])
            key_scales.append(scal[0, slot])
            limit = jnp.where((row16 >> 3) == row, lens[2 * gg + row] - column * BLK, 0)
            live = lane16 < limit
            scores.append(jnp.where(live, s, ABSENT))
            masks.append(live)
        top = functools.reduce(jnp.maximum, scores)
        peak = jnp.max(top, axis=1, keepdims=True)
        total = jnp.zeros((16, BLK), jnp.float32)
        acc = jnp.zeros((16, BLK), jnp.float32)
        for n in range(8):
            t, r = (n // 2) * NGRP + gg, n % 2
            weight = jnp.where(masks[n], jnp.exp(scores[n] - peak), 0.0)
            total = total + weight
            scaled = (weight * value_scales[n]).astype(jnp.bfloat16)
            acc = acc + jnp.dot(scaled, send[t, pl.ds(r * 256 + BLK, BLK), :], preferred_element_type=jnp.float32)
        denom = jnp.sum(total, axis=1, keepdims=True)
        line = jnp.where(lane16 == row16, peak, jnp.where(lane16 == row16 + 16, denom, 0.0))
        line = jnp.sum(line, axis=0, keepdims=True)
        for n in range(8):
            line = jnp.where(lane1 == 32 + 2 * n, key_scales[n], line)
            line = jnp.where(lane1 == 33 + 2 * n, value_scales[n], line)
        smsg[gg] = line
        for qq in range(NSEQ):
            pmsg[qq * NGRP + gg] = acc[4 * qq : 4 * qq + 4].astype(jnp.bfloat16)
        return carry

    lax.fori_loop(0, NGRP, attend, 0)

    for offset in PEERS:
        ty, tg = peer(offset)
        remote(smsg.at[tg], stat.at[me], s_sem, {"seq": ty, "grp": tg}).start()
        remote(pmsg.at[ty * NGRP + tg], part.at[me], p_sem, {"seq": ty, "grp": tg}).start()
    part[me] = pmsg[me]
    stat[me] = smsg[g]
    send_wave(1)
    s_all.wait_recv()
    p_all.wait_recv()

    lines = jnp.broadcast_to(stat[...], (NDEV, 4, BLK))
    row = lax.broadcasted_iota(jnp.int32, (NDEV, 4, BLK), 1) + 4 * y
    lane = lax.broadcasted_iota(jnp.int32, (NDEV, 4, BLK), 2)
    peaks = jnp.sum(jnp.where(lane == row, lines, 0.0), axis=2, keepdims=True)
    sums = jnp.sum(jnp.where(lane == row + 16, lines, 0.0), axis=2, keepdims=True)
    peak = jnp.max(peaks, axis=0, keepdims=True)
    factor = jnp.exp(peaks - peak)
    denom = jnp.sum(sums * factor, axis=0)
    numer = jnp.sum(part[...].astype(jnp.float32) * factor, axis=0)
    rows = (numer / denom).astype(jnp.bfloat16)
    amsg[...] = rows
    att[(y % 2) * 16 + g * 2 + y // 2] = rows

    for offset in PEERS:
        ty, tg = peer(offset)
        remote(amsg, att.at[(y % 2) * 16 + g * 2 + y // 2], a_sem, {"seq": ty, "grp": tg}).start()
    send_wave(2)
    send_wave(3)
    arr[me] = send[me]
    wide = lax.broadcasted_iota(jnp.int32, (8, BLK), 1)
    first = pltpu.roll(jnp.broadcast_to(table[pl.ds(2 * g, 1), :], (8, BLK)), (BLK - 32 * y) % BLK, 1)
    second = pltpu.roll(jnp.broadcast_to(table[pl.ds(2 * g + 1, 1), :], (8, BLK)), (BLK + 32 - 32 * y) % BLK, 1)
    own = jnp.where(wide < 32, first, second)[0:1]
    across = jnp.broadcast_to(own, (BLK, BLK))
    down = across.T
    inside = lax.broadcasted_iota(jnp.int32, (BLK, BLK), 0) < 64
    before = inside & ((down >> 6) == (across >> 6)) & (down < across)
    rank = jnp.sum(before.astype(jnp.int32), axis=0, keepdims=True)
    place_out[...] = ((own >> 6) * 2 + rank) & 63
    owner = lax.broadcasted_iota(jnp.int32, (NDEV, BLK), 0)
    hot = (owner == (own >> 6)).astype(jnp.float32).astype(jnp.bfloat16)
    flat = stat[...].reshape(NDEV, BLK).T.astype(jnp.bfloat16)
    picked = jnp.dot(flat, hot, preferred_element_type=jnp.float32)
    depth = lax.broadcasted_iota(jnp.int32, (BLK, BLK), 0)
    for kv in range(2):
        line = jnp.where(depth == 32 + 4 * y + 2 * rank + kv, picked, 0.0)
        line = jnp.sum(line, axis=0, keepdims=True).astype(jnp.bfloat16)
        scale_out[0, kv : kv + 1, :] = line[:, 0:32]
        scale_out[1, kv : kv + 1, :] = line[:, 32:64]
    w_in.wait()
    a_all.wait_recv()
    attended[...] = att[...].astype(jnp.float32)

    total = jnp.zeros((16, 256), jnp.float32)
    for h in range(8):
        lhs = attended[pl.ds((h // 4) * 16, 16), h % 4, :].astype(jnp.bfloat16)
        total = total + jnp.dot(lhs, w[pl.ds(h * BLK, BLK), :], preferred_element_type=jnp.float32)
    for k in range(NTP):
        pout[k] = total[2 * k : 2 * k + 2]

    for k in range(1, NTP):
        tz = (z + k) % NTP
        remote(pout.at[tz], zbuf.at[z], z_sem, {"tp": tz}).start()
    zbuf[z] = pout[z]
    z_all.wait_recv()
    out_ref[...] = jnp.sum(zbuf[...], axis=0).astype(jnp.bfloat16)

    for phase in (q_all, s_all, p_all, a_all, z_all, b_all):
        phase.wait_send()
    b_all.wait_recv()


def place_kernel(src, arr, summed, scales, out, out_sum, out_scales, sem):
    small = (
        pltpu.make_async_copy(summed, out_sum, sem.at[1]),
        pltpu.make_async_copy(scales, out_scales, sem.at[2]),
    )
    for copy in small:
        copy.start()

    def put(p, carry):
        pltpu.make_async_copy(arr.at[src[0, p]], out.at[p], sem.at[0]).start()
        return carry

    lax.fori_loop(0, 64, put, 0, unroll=8)
    for copy in small:
        copy.wait()
    pltpu.make_async_copy(arr, out, sem.at[0]).wait()


def per_device(queries, cache_pool, block_scale, block_table, lengths, output_weight):
    vmem = pl.BlockSpec(memory_space=pltpu.VMEM)
    smem = pl.BlockSpec(memory_space=pltpu.SMEM)
    hbm = pl.BlockSpec(memory_space=pltpu.HBM)
    anywhere = pl.BlockSpec(memory_space=pl.ANY)
    dma = pltpu.SemaphoreType.DMA
    arrived, summed, scales, place = pl.pallas_call(
        exchange_kernel,
        out_shape=(
            jax.ShapeDtypeStruct((NDEV, 512, BLK), jnp.bfloat16),
            jax.ShapeDtypeStruct((2, 256), jnp.bfloat16),
            jax.ShapeDtypeStruct((2, 2, 32), jnp.bfloat16),
            jax.ShapeDtypeStruct((1, BLK), jnp.int32),
        ),
        in_specs=[hbm] * 6,
        out_specs=(vmem, vmem, vmem, vmem),
        scratch_shapes=[
            pltpu.VMEM((16, BLK), jnp.int32),
            pltpu.VMEM((2, 64), jnp.bfloat16),
            pltpu.VMEM((16, BLK), jnp.int32),
            pltpu.VMEM((2, 64), jnp.float32),
            pltpu.SMEM((16, BLK), jnp.int32),
            pltpu.SMEM((2, 64), jnp.float32),
            pltpu.SMEM((16,), jnp.int32),
            pltpu.VMEM((64, BLK, BLK), jnp.bfloat16),
            pltpu.VMEM((64, BLK, BLK), jnp.bfloat16),
            pltpu.VMEM((NDEV, 512, BLK), jnp.bfloat16),
            pltpu.VMEM((16, BLK), jnp.bfloat16),
            pltpu.VMEM((NGRP, 16, BLK), jnp.bfloat16),
            pltpu.VMEM((1024, 256), jnp.bfloat16),
            pltpu.VMEM((NDEV, 4, BLK), jnp.bfloat16),
            pltpu.VMEM((NDEV, 4, BLK), jnp.bfloat16),
            pltpu.VMEM((NGRP, 1, BLK), jnp.float32),
            pltpu.VMEM((NDEV, 1, BLK), jnp.float32),
            pltpu.VMEM((4, BLK), jnp.bfloat16),
            pltpu.VMEM((NDEV, 4, BLK), jnp.bfloat16),
            pltpu.VMEM((NDEV, 4, BLK), jnp.float32),
            pltpu.VMEM((NTP, 2, 256), jnp.float32),
            pltpu.VMEM((NTP, 2, 256), jnp.float32),
            dma((9,)), dma((2,)), dma((2,)), dma((2,)), dma((2,)), dma((2,)), dma((2,)),
        ],
        compiler_params=pltpu.CompilerParams(
            collective_id=0, has_side_effects=True, vmem_limit_bytes=24 << 20
        ),
    )(*(
        pltpu.with_memory_space_constraint(operand, pltpu.HBM)
        for operand in (
            block_table, lengths, block_scale.reshape(64, 2).T, cache_pool.reshape(64, 256, BLK),
            queries.reshape(16, BLK), output_weight,
        )
    ))
    decode_cache, attention_output, decode_scale = pl.pallas_call(
        place_kernel,
        out_shape=(
            jax.ShapeDtypeStruct((64, 256, BLK), jnp.bfloat16),
            jax.ShapeDtypeStruct((2, 256), jnp.bfloat16),
            jax.ShapeDtypeStruct((2, 2, 32), jnp.bfloat16),
        ),
        in_specs=[smem, vmem, vmem, vmem],
        out_specs=(hbm, hbm, hbm),
        scratch_shapes=[dma((3,))],
        compiler_params=pltpu.CompilerParams(vmem_limit_bytes=12 << 20),
    )(place, arrived.reshape(64, 256, BLK), summed, scales)
    return (
        attention_output,
        decode_cache.reshape(2, 32, 1, 2, BLK, BLK),
        decode_scale.transpose(0, 2, 1).reshape(2, 32, 1, 2),
    )


def solution(mesh):
    placed = (
        P("grp", "tp", None),
        P(("seq", "grp"), "tp", None, None, None),
        P(("seq", "grp"), "tp", None),
        P(),
        P(),
        P("tp", ("seq", "grp")),
    )
    return jax.shard_map(
        per_device,
        mesh=mesh,
        in_specs=placed,
        out_specs=(
            P("tp", ("seq", "grp")),
            P("grp", "seq", "tp", None, None, None),
            P("grp", "seq", "tp", None),
        ),
        check_vma=False,
    )
```

```python
import functools
import math

import jax
import jax.numpy as jnp
from jax import lax
from jax.experimental import pallas as pl
from jax.experimental.pallas import tpu as pltpu
from jax.sharding import PartitionSpec as P

MESH = pl.DeviceIdType.MESH
ABSENT = -1e30
NSEQ, NTP, NGRP = 4, 8, 8
NDEV = NSEQ * NGRP
BLK = 128
ROOT = 1.0 / math.sqrt(128.0)
START = (0, 256, 128, 384)


PEERS = [
    (dy, (dy + turn) % 4, dc)
    for turn in range(4) for dy in range(4) for dc in range(2)
    if (dy, turn, dc) != (0, 0, 0)
]


def exchange_kernel(
    table_hbm, lengths_hbm, scale_hbm, pool_hbm, q_hbm, w_hbm,
    arr, out_ref, scale_out, place_out,
    table, scale_in, codes_v, scales_v, codes, scal, lens,
    pool_k, pool_v, send, q_ref, qall, w, pmsg, part, smsg, stat, amsg, att, attended, pout, zbuf,
    climb, descend, in_sem, q_sem, b_sem, p_sem, s_sem, a_sem, z_sem,
):
    y = lax.axis_index("seq")
    z = lax.axis_index("tp")
    g = lax.axis_index("grp")
    me = y * NGRP + g

    ys = [(y + k) % NSEQ for k in range(NSEQ)]
    xs = [((g // 2 + k) % 4) * 2 for k in range(4)]
    cs = [(g + k) % 2 for k in range(2)]

    def peer(offset):
        dy, dx, dc = offset
        return ys[dy], xs[dx] + cs[dc]

    table_in = pltpu.make_async_copy(table_hbm, table, in_sem.at[0])
    keys_in = pltpu.make_async_copy(pool_hbm.at[:, pl.ds(0, BLK)], pool_k, in_sem.at[1])
    vals_in = pltpu.make_async_copy(pool_hbm.at[:, pl.ds(BLK, BLK)], pool_v, in_sem.at[2])
    q_in = pltpu.make_async_copy(q_hbm, q_ref, in_sem.at[3])
    scales_in = pltpu.make_async_copy(scale_hbm, scale_in, in_sem.at[4])
    lens_in = pltpu.make_async_copy(lengths_hbm, lens, in_sem.at[5])
    w_in = pltpu.make_async_copy(w_hbm, w, in_sem.at[6])
    codes_out = pltpu.make_async_copy(codes_v, codes, in_sem.at[7])
    scales_out = pltpu.make_async_copy(scales_v, scal, in_sem.at[8])
    for copy in (table_in, q_in, keys_in, scales_in, lens_in, vals_in, w_in):
        copy.start()

    barrier = pltpu.get_barrier_semaphore()
    for offset in PEERS:
        ty, tg = peer(offset)
        pl.semaphore_signal(barrier, inc=1, device_id={"seq": ty, "grp": tg}, device_id_type=MESH)
    above, below = z < NTP - 1, z > 0

    @pl.when(above)
    def _():
        pl.semaphore_signal(barrier, inc=1, device_id={"tp": z + 1}, device_id_type=MESH)

    @pl.when(below)
    def _():
        pl.semaphore_signal(barrier, inc=1, device_id={"tp": z - 1}, device_id_type=MESH)

    row16 = lax.broadcasted_iota(jnp.int32, (16, BLK), 0)
    lane16 = lax.broadcasted_iota(jnp.int32, (16, BLK), 1)
    table_in.wait()
    names = table[...]
    code = (names & 63) * 64 + (row16 & 1) * 32 + (lane16 & 31)
    mine = (names >> 6) == me
    low = jnp.where(mine, code, 8191)
    high = jnp.where(mine, code, -1)
    found = jnp.zeros((16, BLK), jnp.int32)
    for qq in range(NSEQ):
        part_of = (lane16 >> 5) == qq
        least = jnp.min(jnp.where(part_of, low, 8191), axis=1, keepdims=True)
        most = jnp.max(jnp.where(part_of, high, -1), axis=1, keepdims=True)
        found = jnp.where(lane16 == qq, least, jnp.where(lane16 == 4 + qq, most, found))
    other = pltpu.roll(found, 15, 0)
    codes_v[...] = jnp.where(lane16 < 4, jnp.minimum(found, other), jnp.maximum(found, other))
    codes_out.start()
    q_in.wait()
    qall[g] = q_ref[...]
    scales_in.wait()
    scales_v[...] = scale_in[...].astype(jnp.float32)
    scales_out.start()
    codes_out.wait()

    def code_of(q, gg, r):
        return codes[2 * gg, q + 4 * r]

    def pick_one(c, ty, tg):
        pool, r = (pool_k, pool_v)[c // 2], c % 2
        slot = (code_of(ty, tg, r) >> 6) & 63
        send[ty * NGRP + tg, pl.ds(START[c], BLK), :] = pool[slot]

    def pick(c):
        pool, r = (pool_k, pool_v)[c // 2], c % 2

        def body(t, carry):
            slot = (code_of(t // NGRP, t % NGRP, r) >> 6) & 63
            send[t, pl.ds(START[c], BLK), :] = pool[slot]
            return carry

        lax.fori_loop(0, NDEV, body, 0)

    def remote(src, dst, sems, device):
        return pltpu.make_async_remote_copy(
            src_ref=src, dst_ref=dst, send_sem=sems.at[0], recv_sem=sems.at[1],
            device_id=device, device_id_type=MESH,
        )

    def send_wave(c):
        rows = pl.ds(START[c], BLK)
        for offset in PEERS:
            ty, tg = peer(offset)
            remote(send.at[ty * NGRP + tg, rows], arr.at[me, rows], b_sem, {"seq": ty, "grp": tg}).start()

    here = {"seq": ys[1]}
    rest = pl.ds(0, NDEV - 1)
    q_all = remote(qall.at[pl.ds(0, NGRP - 1)], qall.at[pl.ds(0, NGRP - 1)], q_sem, here)
    b_all = remote(send.at[rest], arr.at[rest], b_sem, here)
    p_all = remote(pmsg.at[rest], part.at[rest], p_sem, here)
    s_all = remote(stat.at[rest], stat.at[rest], s_sem, here)
    a_all = remote(att.at[rest], att.at[rest], a_sem, here)
    z_all = remote(pout.at[pl.ds(0, NTP - 1)], zbuf.at[pl.ds(0, NTP - 1)], z_sem, here)

    keys_in.wait()
    for offset in PEERS:
        pick_one(0, *peer(offset))
    pl.semaphore_wait(barrier, NDEV - 1 + jnp.where(above, 1, 0) + jnp.where(below, 1, 0))
    for k in range(1, NGRP):
        remote(q_ref, qall.at[g], q_sem, {"grp": (g + k) % NGRP}).start()
    send_wave(0)
    pick_one(0, y, g)
    pick(1)
    vals_in.wait()
    pick(2)
    pick(3)
    scales_out.wait()
    lens_in.wait()
    q_all.wait_recv()

    lane1 = lax.broadcasted_iota(jnp.int32, (1, BLK), 1)

    def attend(gg, carry):
        q = qall[gg]
        scores, masks, key_scales, value_scales = [], [], [], []
        for n in range(8):
            t, r = (n // 2) * NGRP + gg, n % 2
            found_at = code_of(n // 2, gg, r)
            slot, row, column = (found_at >> 6) & 63, (found_at >> 5) & 1, (n // 2) * 32 + (found_at & 31)
            keys = send[t, pl.ds(r * 256, BLK), :]
            s = lax.dot_general(q, keys, (((1,), (1,)), ((), ())), preferred_element_type=jnp.float32)
            s = s * (scal[0, slot] * ROOT)
            value_scales.append(scal[1, slot])
            key_scales.append(scal[0, slot])
            limit = jnp.where((row16 >> 3) == row, lens[2 * gg + row] - column * BLK, 0)
            live = lane16 < limit
            scores.append(jnp.where(live, s, ABSENT))
            masks.append(live)
        top = functools.reduce(jnp.maximum, scores)
        peak = jnp.max(top, axis=1, keepdims=True)
        total = jnp.zeros((16, BLK), jnp.float32)
        acc = jnp.zeros((16, BLK), jnp.float32)
        for n in range(8):
            t, r = (n // 2) * NGRP + gg, n % 2
            weight = jnp.where(masks[n], jnp.exp(scores[n] - peak), 0.0)
            total = total + weight
            scaled = (weight * value_scales[n]).astype(jnp.bfloat16)
            acc = acc + jnp.dot(scaled, send[t, pl.ds(r * 256 + BLK, BLK), :], preferred_element_type=jnp.float32)
        denom = jnp.sum(total, axis=1, keepdims=True)
        line = jnp.where(lane16 == row16, peak, jnp.where(lane16 == row16 + 16, denom, 0.0))
        line = jnp.sum(line, axis=0, keepdims=True)
        for n in range(8):
            line = jnp.where(lane1 == 32 + 2 * n, key_scales[n], line)
            line = jnp.where(lane1 == 33 + 2 * n, value_scales[n], line)
        smsg[gg] = line
        for qq in range(NSEQ):
            pmsg[qq * NGRP + gg] = acc[4 * qq : 4 * qq + 4].astype(jnp.bfloat16)
        return carry

    lax.fori_loop(0, NGRP, attend, 0)

    for offset in PEERS:
        ty, tg = peer(offset)
        remote(smsg.at[tg], stat.at[me], s_sem, {"seq": ty, "grp": tg}).start()
        remote(pmsg.at[ty * NGRP + tg], part.at[me], p_sem, {"seq": ty, "grp": tg}).start()
    part[me] = pmsg[me]
    stat[me] = smsg[g]
    send_wave(1)
    s_all.wait_recv()
    p_all.wait_recv()

    lines = jnp.broadcast_to(stat[...], (NDEV, 4, BLK))
    row = lax.broadcasted_iota(jnp.int32, (NDEV, 4, BLK), 1) + 4 * y
    lane = lax.broadcasted_iota(jnp.int32, (NDEV, 4, BLK), 2)
    peaks = jnp.sum(jnp.where(lane == row, lines, 0.0), axis=2, keepdims=True)
    sums = jnp.sum(jnp.where(lane == row + 16, lines, 0.0), axis=2, keepdims=True)
    peak = jnp.max(peaks, axis=0, keepdims=True)
    factor = jnp.exp(peaks - peak)
    denom = jnp.sum(sums * factor, axis=0)
    numer = jnp.sum(part[...].astype(jnp.float32) * factor, axis=0)
    rows = (numer / denom).astype(jnp.bfloat16)
    amsg[...] = rows
    att[(y % 2) * 16 + g * 2 + y // 2] = rows

    for offset in PEERS:
        ty, tg = peer(offset)
        remote(amsg, att.at[(y % 2) * 16 + g * 2 + y // 2], a_sem, {"seq": ty, "grp": tg}).start()
    send_wave(2)
    send_wave(3)
    arr[me] = send[me]
    wide = lax.broadcasted_iota(jnp.int32, (8, BLK), 1)
    first = pltpu.roll(jnp.broadcast_to(table[pl.ds(2 * g, 1), :], (8, BLK)), (BLK - 32 * y) % BLK, 1)
    second = pltpu.roll(jnp.broadcast_to(table[pl.ds(2 * g + 1, 1), :], (8, BLK)), (BLK + 32 - 32 * y) % BLK, 1)
    own = jnp.where(wide < 32, first, second)[0:1]
    across = jnp.broadcast_to(own, (BLK, BLK))
    down = across.T
    inside = lax.broadcasted_iota(jnp.int32, (BLK, BLK), 0) < 64
    before = inside & ((down >> 6) == (across >> 6)) & (down < across)
    rank = jnp.sum(before.astype(jnp.int32), axis=0, keepdims=True)
    place_out[...] = ((own >> 6) * 2 + rank) & 63
    owner = lax.broadcasted_iota(jnp.int32, (NDEV, BLK), 0)
    hot = (owner == (own >> 6)).astype(jnp.float32).astype(jnp.bfloat16)
    flat = stat[...].reshape(NDEV, BLK).T.astype(jnp.bfloat16)
    picked = jnp.dot(flat, hot, preferred_element_type=jnp.float32)
    depth = lax.broadcasted_iota(jnp.int32, (BLK, BLK), 0)
    for kv in range(2):
        line = jnp.where(depth == 32 + 4 * y + 2 * rank + kv, picked, 0.0)
        line = jnp.sum(line, axis=0, keepdims=True).astype(jnp.bfloat16)
        scale_out[0, kv : kv + 1, :] = line[:, 0:32]
        scale_out[1, kv : kv + 1, :] = line[:, 32:64]
    @pl.when(below)
    def _():
        pl.semaphore_wait(climb, 1)

    @pl.when(above)
    def _():
        pl.semaphore_signal(climb, inc=1, device_id={"tp": z + 1}, device_id_type=MESH)
        pl.semaphore_wait(descend, 1)

    @pl.when(below)
    def _():
        pl.semaphore_signal(descend, inc=1, device_id={"tp": z - 1}, device_id_type=MESH)

    w_in.wait()
    a_all.wait_recv()
    attended[...] = att[...].astype(jnp.float32)

    total = jnp.zeros((16, 256), jnp.float32)
    for h in range(8):
        lhs = attended[pl.ds((h // 4) * 16, 16), h % 4, :].astype(jnp.bfloat16)
        total = total + jnp.dot(lhs, w[pl.ds(h * BLK, BLK), :], preferred_element_type=jnp.float32)
    for k in range(NTP):
        pout[k] = total[2 * k : 2 * k + 2]

    for k in range(1, NTP):
        tz = (z + k) % NTP
        remote(pout.at[tz], zbuf.at[z], z_sem, {"tp": tz}).start()
    zbuf[z] = pout[z]
    z_all.wait_recv()
    out_ref[...] = jnp.sum(zbuf[...], axis=0).astype(jnp.bfloat16)

    for phase in (q_all, s_all, p_all, a_all, z_all, b_all):
        phase.wait_send()
    b_all.wait_recv()


def place_kernel(src, arr, summed, scales, out, out_sum, out_scales, sem):
    small = (
        pltpu.make_async_copy(summed, out_sum, sem.at[1]),
        pltpu.make_async_copy(scales, out_scales, sem.at[2]),
    )
    for copy in small:
        copy.start()

    def put(p, carry):
        pltpu.make_async_copy(arr.at[src[0, p]], out.at[p], sem.at[0]).start()
        return carry

    lax.fori_loop(0, 64, put, 0, unroll=8)
    for copy in small:
        copy.wait()
    pltpu.make_async_copy(arr, out, sem.at[0]).wait()


def per_device(queries, cache_pool, block_scale, block_table, lengths, output_weight):
    vmem = pl.BlockSpec(memory_space=pltpu.VMEM)
    smem = pl.BlockSpec(memory_space=pltpu.SMEM)
    hbm = pl.BlockSpec(memory_space=pltpu.HBM)
    anywhere = pl.BlockSpec(memory_space=pl.ANY)
    dma = pltpu.SemaphoreType.DMA
    arrived, summed, scales, place = pl.pallas_call(
        exchange_kernel,
        out_shape=(
            jax.ShapeDtypeStruct((NDEV, 512, BLK), jnp.bfloat16),
            jax.ShapeDtypeStruct((2, 256), jnp.bfloat16),
            jax.ShapeDtypeStruct((2, 2, 32), jnp.bfloat16),
            jax.ShapeDtypeStruct((1, BLK), jnp.int32),
        ),
        in_specs=[hbm] * 6,
        out_specs=(vmem, vmem, vmem, vmem),
        scratch_shapes=[
            pltpu.VMEM((16, BLK), jnp.int32),
            pltpu.VMEM((2, 64), jnp.bfloat16),
            pltpu.VMEM((16, BLK), jnp.int32),
            pltpu.VMEM((2, 64), jnp.float32),
            pltpu.SMEM((16, BLK), jnp.int32),
            pltpu.SMEM((2, 64), jnp.float32),
            pltpu.SMEM((16,), jnp.int32),
            pltpu.VMEM((64, BLK, BLK), jnp.bfloat16),
            pltpu.VMEM((64, BLK, BLK), jnp.bfloat16),
            pltpu.VMEM((NDEV, 512, BLK), jnp.bfloat16),
            pltpu.VMEM((16, BLK), jnp.bfloat16),
            pltpu.VMEM((NGRP, 16, BLK), jnp.bfloat16),
            pltpu.VMEM((1024, 256), jnp.bfloat16),
            pltpu.VMEM((NDEV, 4, BLK), jnp.bfloat16),
            pltpu.VMEM((NDEV, 4, BLK), jnp.bfloat16),
            pltpu.VMEM((NGRP, 1, BLK), jnp.float32),
            pltpu.VMEM((NDEV, 1, BLK), jnp.float32),
            pltpu.VMEM((4, BLK), jnp.bfloat16),
            pltpu.VMEM((NDEV, 4, BLK), jnp.bfloat16),
            pltpu.VMEM((NDEV, 4, BLK), jnp.float32),
            pltpu.VMEM((NTP, 2, 256), jnp.float32),
            pltpu.VMEM((NTP, 2, 256), jnp.float32),
            pltpu.SemaphoreType.REGULAR, pltpu.SemaphoreType.REGULAR,
            dma((9,)), dma((2,)), dma((2,)), dma((2,)), dma((2,)), dma((2,)), dma((2,)),
        ],
        compiler_params=pltpu.CompilerParams(
            collective_id=0, has_side_effects=True, vmem_limit_bytes=24 << 20
        ),
    )(*(
        pltpu.with_memory_space_constraint(operand, pltpu.HBM)
        for operand in (
            block_table, lengths, block_scale.reshape(64, 2).T, cache_pool.reshape(64, 256, BLK),
            queries.reshape(16, BLK), output_weight,
        )
    ))
    decode_cache, attention_output, decode_scale = pl.pallas_call(
        place_kernel,
        out_shape=(
            jax.ShapeDtypeStruct((64, 256, BLK), jnp.bfloat16),
            jax.ShapeDtypeStruct((2, 256), jnp.bfloat16),
            jax.ShapeDtypeStruct((2, 2, 32), jnp.bfloat16),
        ),
        in_specs=[smem, vmem, vmem, vmem],
        out_specs=(hbm, hbm, hbm),
        scratch_shapes=[dma((3,))],
        compiler_params=pltpu.CompilerParams(vmem_limit_bytes=12 << 20),
    )(place, arrived.reshape(64, 256, BLK), summed, scales)
    return (
        attention_output,
        decode_cache.reshape(2, 32, 1, 2, BLK, BLK),
        decode_scale.transpose(0, 2, 1).reshape(2, 32, 1, 2),
    )


def solution(mesh):
    placed = (
        P("grp", "tp", None),
        P(("seq", "grp"), "tp", None, None, None),
        P(("seq", "grp"), "tp", None),
        P(),
        P(),
        P("tp", ("seq", "grp")),
    )
    return jax.shard_map(
        per_device,
        mesh=mesh,
        in_specs=placed,
        out_specs=(
            P("tp", ("seq", "grp")),
            P("grp", "seq", "tp", None, None, None),
            P("grp", "seq", "tp", None),
        ),
        check_vma=False,
    )
```

```python
import functools
import math

import jax
import jax.numpy as jnp
from jax import lax
from jax.experimental import pallas as pl
from jax.experimental.pallas import tpu as pltpu
from jax.sharding import PartitionSpec as P

MESH = pl.DeviceIdType.MESH
ABSENT = -1e30
NSEQ, NTP, NGRP = 4, 8, 8
NDEV = NSEQ * NGRP
BLK = 128
ROOT = 1.0 / math.sqrt(128.0)
HALF = 64
PEERS = [
    (dy, (dy + turn) % 4, dc)
    for turn in range(4) for dy in range(4) for dc in range(2)
    if (dy, turn, dc) != (0, 0, 0)
]


def exchange_kernel(
    table_hbm, lengths_hbm, scale_hbm, pool_hbm, q_hbm, w_hbm,
    out, out_ref, scale_out,
    table, scale_in, codes_v, scales_v, codes, scal, lens,
    place_v, place, pool_k, pool_v, send_k, send_v0, send_v1, arr_k, arr_v0, arr_v1, q_ref, qall, w, pmsg, part, smsg, stat, amsg, att, attended, pout, zbuf,
    climb, descend, in_sem, q_sem, k_sem, v0_sem, v1_sem, p_sem, s_sem, a_sem, z_sem,
):
    y = lax.axis_index("seq")
    z = lax.axis_index("tp")
    g = lax.axis_index("grp")
    me = y * NGRP + g

    ys = [(y + k) % NSEQ for k in range(NSEQ)]
    xs = [((g // 2 + k) % 4) * 2 for k in range(4)]
    cs = [(g + k) % 2 for k in range(2)]

    def peer(offset):
        dy, dx, dc = offset
        return ys[dy], xs[dx] + cs[dc]

    table_in = pltpu.make_async_copy(table_hbm, table, in_sem.at[0])
    keys_in = pltpu.make_async_copy(pool_hbm.at[:, pl.ds(0, BLK)], pool_k, in_sem.at[1])
    vals_in = pltpu.make_async_copy(pool_hbm.at[:, pl.ds(BLK, BLK)], pool_v, in_sem.at[2])
    q_in = pltpu.make_async_copy(q_hbm, q_ref, in_sem.at[3])
    scales_in = pltpu.make_async_copy(scale_hbm, scale_in, in_sem.at[4])
    lens_in = pltpu.make_async_copy(lengths_hbm, lens, in_sem.at[5])
    w_in = pltpu.make_async_copy(w_hbm, w, in_sem.at[6])
    codes_out = pltpu.make_async_copy(codes_v, codes, in_sem.at[7])
    scales_out = pltpu.make_async_copy(scales_v, scal, in_sem.at[8])
    place_in = pltpu.make_async_copy(place_v, place, in_sem.at[9])
    for copy in (table_in, keys_in, q_in, scales_in, lens_in):
        copy.start()

    barrier = pltpu.get_barrier_semaphore()
    for offset in PEERS:
        ty, tg = peer(offset)
        pl.semaphore_signal(barrier, inc=1, device_id={"seq": ty, "grp": tg}, device_id_type=MESH)
    above, below = z < NTP - 1, z > 0

    @pl.when(above)
    def _():
        pl.semaphore_signal(barrier, inc=1, device_id={"tp": z + 1}, device_id_type=MESH)

    @pl.when(below)
    def _():
        pl.semaphore_signal(barrier, inc=1, device_id={"tp": z - 1}, device_id_type=MESH)

    row16 = lax.broadcasted_iota(jnp.int32, (16, BLK), 0)
    lane16 = lax.broadcasted_iota(jnp.int32, (16, BLK), 1)
    table_in.wait()
    names = table[...]
    code = (names & 63) * 64 + (row16 & 1) * 32 + (lane16 & 31)
    mine = (names >> 6) == me
    low = jnp.where(mine, code, 8191)
    high = jnp.where(mine, code, -1)
    found = jnp.zeros((16, BLK), jnp.int32)
    for qq in range(NSEQ):
        part_of = (lane16 >> 5) == qq
        least = jnp.min(jnp.where(part_of, low, 8191), axis=1, keepdims=True)
        most = jnp.max(jnp.where(part_of, high, -1), axis=1, keepdims=True)
        found = jnp.where(lane16 == qq, least, jnp.where(lane16 == 4 + qq, most, found))
    other = pltpu.roll(found, 15, 0)
    codes_v[...] = jnp.where(lane16 < 4, jnp.minimum(found, other), jnp.maximum(found, other))
    codes_out.start()
    q_in.wait()
    qall[g] = q_ref[...]
    scales_in.wait()
    scales_v[...] = scale_in[...].astype(jnp.float32)
    scales_out.start()
    codes_out.wait()

    def code_of(q, gg, r):
        return codes[2 * gg, q + 4 * r]

    def slot_of(ty, tg, r):
        return (code_of(ty, tg, r) >> 6) & 63

    def pick_keys(r, ty, tg):
        send_k[2 * (ty * NGRP + tg) + r] = pool_k[slot_of(ty, tg, r)]

    def pick_values(t, carry):
        for r in range(2):
            slot = slot_of(t // NGRP, t % NGRP, r)
            send_v0[2 * t + r] = pool_v[slot, pl.ds(0, HALF), :]
            send_v1[2 * t + r] = pool_v[slot, pl.ds(HALF, HALF), :]
        return carry

    def remote(src, dst, sems, device):
        return pltpu.make_async_remote_copy(
            src_ref=src, dst_ref=dst, send_sem=sems.at[0], recv_sem=sems.at[1],
            device_id=device, device_id_type=MESH,
        )

    def send_keys(r, ty, tg):
        device = {"seq": ty, "grp": tg}
        remote(send_k.at[2 * (ty * NGRP + tg) + r], arr_k.at[2 * me + r], k_sem, device).start()

    def send_values(src, dst, sems):
        for offset in PEERS:
            ty, tg = peer(offset)
            theirs, mine = pl.ds(2 * (ty * NGRP + tg), 2), pl.ds(2 * me, 2)
            remote(src.at[theirs], dst.at[mine], sems, {"seq": ty, "grp": tg}).start()

    here = {"seq": ys[1]}
    rest = pl.ds(0, NDEV - 1)
    q_all = remote(qall.at[pl.ds(0, NGRP - 1)], qall.at[pl.ds(0, NGRP - 1)], q_sem, here)
    both = pl.ds(0, 2 * (NDEV - 1))
    k_all = remote(send_k.at[both], arr_k.at[both], k_sem, here)
    v0_all = remote(send_v0.at[both], arr_v0.at[both], v0_sem, here)
    v1_all = remote(send_v1.at[both], arr_v1.at[both], v1_sem, here)
    p_all = remote(pmsg.at[rest], part.at[rest], p_sem, here)
    s_all = remote(stat.at[rest], stat.at[rest], s_sem, here)
    a_all = remote(att.at[rest], att.at[rest], a_sem, here)
    z_all = remote(pout.at[pl.ds(0, NTP - 1)], zbuf.at[pl.ds(0, NTP - 1)], z_sem, here)

    keys_in.wait()
    vals_in.start()
    w_in.start()
    ahead = 6
    for offset in PEERS[:ahead]:
        pick_keys(0, *peer(offset))
    pl.semaphore_wait(barrier, NDEV - 1 + jnp.where(above, 1, 0) + jnp.where(below, 1, 0))
    for k in range(1, NGRP):
        remote(q_ref, qall.at[g], q_sem, {"grp": (g + k) % NGRP}).start()
    for i, offset in enumerate(PEERS):
        if i + ahead < len(PEERS):
            pick_keys(0, *peer(PEERS[i + ahead]))
        send_keys(0, *peer(offset))
    pick_keys(0, y, g)
    for offset in PEERS + [(0, 0, 0)]:
        pick_keys(1, *peer(offset))
    vals_in.wait()
    lax.fori_loop(0, NDEV, pick_values, 0)
    scales_out.wait()
    lens_in.wait()
    q_all.wait_recv()

    lane1 = lax.broadcasted_iota(jnp.int32, (1, BLK), 1)

    def attend(gg, carry):
        q = qall[gg]
        scores, masks, key_scales, value_scales = [], [], [], []
        for n in range(8):
            t, r = (n // 2) * NGRP + gg, n % 2
            found_at = code_of(n // 2, gg, r)
            slot, row, column = (found_at >> 6) & 63, (found_at >> 5) & 1, (n // 2) * 32 + (found_at & 31)
            keys = send_k[2 * t + r]
            s = lax.dot_general(q, keys, (((1,), (1,)), ((), ())), preferred_element_type=jnp.float32)
            s = s * (scal[0, slot] * ROOT)
            value_scales.append(scal[1, slot])
            key_scales.append(scal[0, slot])
            limit = jnp.where((row16 >> 3) == row, lens[2 * gg + row] - column * BLK, 0)
            live = lane16 < limit
            scores.append(jnp.where(live, s, ABSENT))
            masks.append(live)
        top = functools.reduce(jnp.maximum, scores)
        peak = jnp.max(top, axis=1, keepdims=True)
        total = jnp.zeros((16, BLK), jnp.float32)
        acc = jnp.zeros((16, BLK), jnp.float32)
        for n in range(8):
            t, r = (n // 2) * NGRP + gg, n % 2
            weight = jnp.where(masks[n], jnp.exp(scores[n] - peak), 0.0)
            total = total + weight
            scaled = (weight * value_scales[n]).astype(jnp.bfloat16)
            values = jnp.concatenate([send_v0[2 * t + r], send_v1[2 * t + r]], axis=0)
            acc = acc + jnp.dot(scaled, values, preferred_element_type=jnp.float32)
        denom = jnp.sum(total, axis=1, keepdims=True)
        line = jnp.where(lane16 == row16, peak, jnp.where(lane16 == row16 + 16, denom, 0.0))
        line = jnp.sum(line, axis=0, keepdims=True)
        for n in range(8):
            line = jnp.where(lane1 == 32 + 2 * n, key_scales[n], line)
            line = jnp.where(lane1 == 33 + 2 * n, value_scales[n], line)
        smsg[gg] = line
        for qq in range(NSEQ):
            pmsg[qq * NGRP + gg] = acc[4 * qq : 4 * qq + 4].astype(jnp.bfloat16)
        return carry

    lax.fori_loop(0, NGRP, attend, 0)

    for offset in PEERS:
        ty, tg = peer(offset)
        remote(smsg.at[tg], stat.at[me], s_sem, {"seq": ty, "grp": tg}).start()
        remote(pmsg.at[ty * NGRP + tg], part.at[me], p_sem, {"seq": ty, "grp": tg}).start()
    part[me] = pmsg[me]
    stat[me] = smsg[g]
    for offset in PEERS:
        send_keys(1, *peer(offset))
    s_all.wait_recv()
    p_all.wait_recv()

    lines = jnp.broadcast_to(stat[...], (NDEV, 4, BLK))
    row = lax.broadcasted_iota(jnp.int32, (NDEV, 4, BLK), 1) + 4 * y
    lane = lax.broadcasted_iota(jnp.int32, (NDEV, 4, BLK), 2)
    peaks = jnp.sum(jnp.where(lane == row, lines, 0.0), axis=2, keepdims=True)
    sums = jnp.sum(jnp.where(lane == row + 16, lines, 0.0), axis=2, keepdims=True)
    peak = jnp.max(peaks, axis=0, keepdims=True)
    factor = jnp.exp(peaks - peak)
    denom = jnp.sum(sums * factor, axis=0)
    numer = jnp.sum(part[...].astype(jnp.float32) * factor, axis=0)
    rows = (numer / denom).astype(jnp.bfloat16)
    amsg[...] = rows
    att[(y % 2) * 16 + g * 2 + y // 2] = rows

    for offset in PEERS:
        ty, tg = peer(offset)
        remote(amsg, att.at[(y % 2) * 16 + g * 2 + y // 2], a_sem, {"seq": ty, "grp": tg}).start()
    send_values(send_v0, arr_v0, v0_sem)
    send_values(send_v1, arr_v1, v1_sem)
    for sent, arrived in ((send_k, arr_k), (send_v0, arr_v0), (send_v1, arr_v1)):
        arrived[pl.ds(2 * me, 2)] = sent[pl.ds(2 * me, 2)]
    wide = lax.broadcasted_iota(jnp.int32, (8, BLK), 1)
    first = pltpu.roll(jnp.broadcast_to(table[pl.ds(2 * g, 1), :], (8, BLK)), (BLK - 32 * y) % BLK, 1)
    second = pltpu.roll(jnp.broadcast_to(table[pl.ds(2 * g + 1, 1), :], (8, BLK)), (BLK + 32 - 32 * y) % BLK, 1)
    own = jnp.where(wide < 32, first, second)[0:1]
    across = jnp.broadcast_to(own, (BLK, BLK))
    down = across.T
    inside = lax.broadcasted_iota(jnp.int32, (BLK, BLK), 0) < 64
    before = inside & ((down >> 6) == (across >> 6)) & (down < across)
    rank = jnp.sum(before.astype(jnp.int32), axis=0, keepdims=True)
    place_v[...] = ((own >> 6) * 2 + rank) & 63
    place_in.start()
    owner = lax.broadcasted_iota(jnp.int32, (NDEV, BLK), 0)
    hot = (owner == (own >> 6)).astype(jnp.float32).astype(jnp.bfloat16)
    flat = stat[...].reshape(NDEV, BLK).T.astype(jnp.bfloat16)
    picked = jnp.dot(flat, hot, preferred_element_type=jnp.float32)
    depth = lax.broadcasted_iota(jnp.int32, (BLK, BLK), 0)
    for kv in range(2):
        line = jnp.where(depth == 32 + 4 * y + 2 * rank + kv, picked, 0.0)
        line = jnp.sum(line, axis=0, keepdims=True).astype(jnp.bfloat16)
        scale_out[0, kv : kv + 1, :] = line[:, 0:32]
        scale_out[1, kv : kv + 1, :] = line[:, 32:64]
    @pl.when(below)
    def _():
        pl.semaphore_wait(climb, 1)

    @pl.when(above)
    def _():
        pl.semaphore_signal(climb, inc=1, device_id={"tp": z + 1}, device_id_type=MESH)
        pl.semaphore_wait(descend, 1)

    @pl.when(below)
    def _():
        pl.semaphore_signal(descend, inc=1, device_id={"tp": z - 1}, device_id_type=MESH)

    w_in.wait()
    a_all.wait_recv()
    attended[...] = att[...].astype(jnp.float32)

    total = jnp.zeros((16, 256), jnp.float32)
    for h in range(8):
        lhs = attended[pl.ds((h // 4) * 16, 16), h % 4, :].astype(jnp.bfloat16)
        total = total + jnp.dot(lhs, w[pl.ds(h * BLK, BLK), :], preferred_element_type=jnp.float32)
    for k in range(NTP):
        pout[k] = total[2 * k : 2 * k + 2]

    for k in range(1, NTP):
        tz = (z + k) % NTP
        remote(pout.at[tz], zbuf.at[z], z_sem, {"tp": tz}).start()
    zbuf[z] = pout[z]
    z_all.wait_recv()
    out_ref[...] = jnp.sum(zbuf[...], axis=0).astype(jnp.bfloat16)

    place_in.wait()

    def settle(arrived, start, length):
        def body(p, carry):
            out[p, pl.ds(start, length), :] = arrived[place[0, p]]
            return carry

        lax.fori_loop(0, 64, body, 0, unroll=8)

    k_all.wait_recv()
    settle(arr_k, 0, BLK)
    v0_all.wait_recv()
    settle(arr_v0, BLK, HALF)
    for phase in (q_all, s_all, p_all, a_all, z_all, k_all, v0_all, v1_all):
        phase.wait_send()
    v1_all.wait_recv()
    settle(arr_v1, BLK + HALF, HALF)


def write_kernel(cache, summed, scales, out, out_sum, out_scales, sem):
    copies = [
        pltpu.make_async_copy(cache, out, sem.at[0]),
        pltpu.make_async_copy(summed, out_sum, sem.at[1]),
        pltpu.make_async_copy(scales, out_scales, sem.at[2]),
    ]
    for copy in copies:
        copy.start()
    for copy in copies:
        copy.wait()


def per_device(queries, cache_pool, block_scale, block_table, lengths, output_weight):
    vmem = pl.BlockSpec(memory_space=pltpu.VMEM)
    hbm = pl.BlockSpec(memory_space=pltpu.HBM)
    dma = pltpu.SemaphoreType.DMA
    cache, summed, scales = pl.pallas_call(
        exchange_kernel,
        out_shape=(
            jax.ShapeDtypeStruct((64, 256, BLK), jnp.bfloat16),
            jax.ShapeDtypeStruct((2, 256), jnp.bfloat16),
            jax.ShapeDtypeStruct((2, 2, 32), jnp.bfloat16),
        ),
        in_specs=[hbm] * 6,
        out_specs=(vmem, vmem, vmem),
        scratch_shapes=[
            pltpu.VMEM((16, BLK), jnp.int32),
            pltpu.VMEM((2, 64), jnp.bfloat16),
            pltpu.VMEM((16, BLK), jnp.int32),
            pltpu.VMEM((2, 64), jnp.float32),
            pltpu.SMEM((16, BLK), jnp.int32),
            pltpu.SMEM((2, 64), jnp.float32),
            pltpu.SMEM((16,), jnp.int32),
            pltpu.VMEM((1, BLK), jnp.int32),
            pltpu.SMEM((1, BLK), jnp.int32),
            pltpu.VMEM((64, BLK, BLK), jnp.bfloat16),
            pltpu.VMEM((64, BLK, BLK), jnp.bfloat16),
            pltpu.VMEM((64, BLK, BLK), jnp.bfloat16),
            pltpu.VMEM((64, HALF, BLK), jnp.bfloat16),
            pltpu.VMEM((64, HALF, BLK), jnp.bfloat16),
            pltpu.VMEM((64, BLK, BLK), jnp.bfloat16),
            pltpu.VMEM((64, HALF, BLK), jnp.bfloat16),
            pltpu.VMEM((64, HALF, BLK), jnp.bfloat16),
            pltpu.VMEM((16, BLK), jnp.bfloat16),
            pltpu.VMEM((NGRP, 16, BLK), jnp.bfloat16),
            pltpu.VMEM((1024, 256), jnp.bfloat16),
            pltpu.VMEM((NDEV, 4, BLK), jnp.bfloat16),
            pltpu.VMEM((NDEV, 4, BLK), jnp.bfloat16),
            pltpu.VMEM((NGRP, 1, BLK), jnp.float32),
            pltpu.VMEM((NDEV, 1, BLK), jnp.float32),
            pltpu.VMEM((4, BLK), jnp.bfloat16),
            pltpu.VMEM((NDEV, 4, BLK), jnp.bfloat16),
            pltpu.VMEM((NDEV, 4, BLK), jnp.float32),
            pltpu.VMEM((NTP, 2, 256), jnp.float32),
            pltpu.VMEM((NTP, 2, 256), jnp.float32),
            pltpu.SemaphoreType.REGULAR, pltpu.SemaphoreType.REGULAR,
            dma((10,)), dma((2,)), dma((2,)), dma((2,)), dma((2,)), dma((2,)), dma((2,)), dma((2,)), dma((2,)),
        ],
        compiler_params=pltpu.CompilerParams(
            collective_id=0, has_side_effects=True, vmem_limit_bytes=24 << 20
        ),
    )(*(
        pltpu.with_memory_space_constraint(operand, pltpu.HBM)
        for operand in (
            block_table, lengths, block_scale.reshape(64, 2).T, cache_pool.reshape(64, 256, BLK),
            queries.reshape(16, BLK), output_weight,
        )
    ))
    decode_cache, attention_output, decode_scale = pl.pallas_call(
        write_kernel,
        out_shape=(
            jax.ShapeDtypeStruct((64, 256, BLK), jnp.bfloat16),
            jax.ShapeDtypeStruct((2, 256), jnp.bfloat16),
            jax.ShapeDtypeStruct((2, 2, 32), jnp.bfloat16),
        ),
        in_specs=[vmem, vmem, vmem],
        out_specs=(hbm, hbm, hbm),
        scratch_shapes=[dma((3,))],
        compiler_params=pltpu.CompilerParams(vmem_limit_bytes=12 << 20),
    )(cache, summed, scales)
    return (
        attention_output,
        decode_cache.reshape(2, 32, 1, 2, BLK, BLK),
        decode_scale.transpose(0, 2, 1).reshape(2, 32, 1, 2),
    )


def solution(mesh):
    placed = (
        P("grp", "tp", None),
        P(("seq", "grp"), "tp", None, None, None),
        P(("seq", "grp"), "tp", None),
        P(),
        P(),
        P("tp", ("seq", "grp")),
    )
    return jax.shard_map(
        per_device,
        mesh=mesh,
        in_specs=placed,
        out_specs=(
            P("tp", ("seq", "grp")),
            P("grp", "seq", "tp", None, None, None),
            P("grp", "seq", "tp", None),
        ),
        check_vma=False,
    )
```

```python
import functools
import math

import jax
import jax.numpy as jnp
from jax import lax
from jax.experimental import pallas as pl
from jax.experimental.pallas import tpu as pltpu
from jax.sharding import PartitionSpec as P

MESH = pl.DeviceIdType.MESH
ABSENT = -1e30
NSEQ, NTP, NGRP = 4, 8, 8
NDEV = NSEQ * NGRP
BLK = 128
ROOT = 1.0 / math.sqrt(128.0)
HALF = 64
PEERS = [
    (dy, (dy + turn) % 4, dc)
    for turn in range(4) for dy in range(4) for dc in range(2)
    if (dy, turn, dc) != (0, 0, 0)
]

PEERS = [o for a in PEERS for o in (a, (-a[0] % 4, -a[1] % 4, a[2]))]
PEERS = list(dict.fromkeys(PEERS))


def exchange_kernel(
    table_hbm, lengths_hbm, scale_hbm, pool_hbm, q_hbm, w_hbm,
    out, out_ref, scale_out,
    table, scale_in, codes_v, scales_v, codes, scal, lens,
    place_v, place, pool_k, pool_v, send_k, send_v0, send_v1, arr_k, arr_v0, arr_v1, q_ref, qall, w, pmsg, part, smsg, stat, amsg, att, attended, pout, zbuf,
    climb, descend, in_sem, q_sem, k_sem, v0_sem, v1_sem, p_sem, s_sem, a_sem, z_sem,
):
    y = lax.axis_index("seq")
    z = lax.axis_index("tp")
    g = lax.axis_index("grp")
    me = y * NGRP + g

    ys = [(y + k) % NSEQ for k in range(NSEQ)]
    xs = [((g // 2 + k) % 4) * 2 for k in range(4)]
    cs = [(g + k) % 2 for k in range(2)]

    def peer(offset):
        dy, dx, dc = offset
        return ys[dy], xs[dx] + cs[dc]

    table_in = pltpu.make_async_copy(table_hbm, table, in_sem.at[0])
    keys_in = pltpu.make_async_copy(pool_hbm.at[:, pl.ds(0, BLK)], pool_k, in_sem.at[1])
    vals_in = pltpu.make_async_copy(pool_hbm.at[:, pl.ds(BLK, BLK)], pool_v, in_sem.at[2])
    q_in = pltpu.make_async_copy(q_hbm, q_ref, in_sem.at[3])
    scales_in = pltpu.make_async_copy(scale_hbm, scale_in, in_sem.at[4])
    lens_in = pltpu.make_async_copy(lengths_hbm, lens, in_sem.at[5])
    w_in = pltpu.make_async_copy(w_hbm, w, in_sem.at[6])
    codes_out = pltpu.make_async_copy(codes_v, codes, in_sem.at[7])
    scales_out = pltpu.make_async_copy(scales_v, scal, in_sem.at[8])
    place_in = pltpu.make_async_copy(place_v, place, in_sem.at[9])
    for copy in (table_in, keys_in, q_in, scales_in, lens_in):
        copy.start()

    barrier = pltpu.get_barrier_semaphore()
    for offset in PEERS:
        ty, tg = peer(offset)
        pl.semaphore_signal(barrier, inc=1, device_id={"seq": ty, "grp": tg}, device_id_type=MESH)
    above, below = z < NTP - 1, z > 0

    @pl.when(above)
    def _():
        pl.semaphore_signal(barrier, inc=1, device_id={"tp": z + 1}, device_id_type=MESH)

    @pl.when(below)
    def _():
        pl.semaphore_signal(barrier, inc=1, device_id={"tp": z - 1}, device_id_type=MESH)

    row16 = lax.broadcasted_iota(jnp.int32, (16, BLK), 0)
    lane16 = lax.broadcasted_iota(jnp.int32, (16, BLK), 1)
    table_in.wait()
    names = table[...]
    code = (names & 63) * 64 + (row16 & 1) * 32 + (lane16 & 31)
    mine = (names >> 6) == me
    low = jnp.where(mine, code, 8191)
    high = jnp.where(mine, code, -1)
    found = jnp.zeros((16, BLK), jnp.int32)
    for qq in range(NSEQ):
        part_of = (lane16 >> 5) == qq
        least = jnp.min(jnp.where(part_of, low, 8191), axis=1, keepdims=True)
        most = jnp.max(jnp.where(part_of, high, -1), axis=1, keepdims=True)
        found = jnp.where(lane16 == qq, least, jnp.where(lane16 == 4 + qq, most, found))
    other = pltpu.roll(found, 15, 0)
    codes_v[...] = jnp.where(lane16 < 4, jnp.minimum(found, other), jnp.maximum(found, other))
    codes_out.start()
    q_in.wait()
    qall[g] = q_ref[...]
    scales_in.wait()
    scales_v[...] = scale_in[...].astype(jnp.float32)
    scales_out.start()
    codes_out.wait()

    def code_of(q, gg, r):
        return codes[2 * gg, q + 4 * r]

    def slot_of(ty, tg, r):
        return (code_of(ty, tg, r) >> 6) & 63

    def pick_keys(r, ty, tg):
        send_k[2 * (ty * NGRP + tg) + r] = pool_k[slot_of(ty, tg, r)]

    def pick_values(t, carry):
        for r in range(2):
            slot = slot_of(t // NGRP, t % NGRP, r)
            send_v0[2 * t + r] = pool_v[slot, pl.ds(0, HALF), :]
            send_v1[2 * t + r] = pool_v[slot, pl.ds(HALF, HALF), :]
        return carry

    def remote(src, dst, sems, device):
        return pltpu.make_async_remote_copy(
            src_ref=src, dst_ref=dst, send_sem=sems.at[0], recv_sem=sems.at[1],
            device_id=device, device_id_type=MESH,
        )

    def send_keys(r, ty, tg):
        device = {"seq": ty, "grp": tg}
        remote(send_k.at[2 * (ty * NGRP + tg) + r], arr_k.at[2 * me + r], k_sem, device).start()

    def send_values(src, dst, sems):
        for offset in PEERS:
            ty, tg = peer(offset)
            theirs, mine = pl.ds(2 * (ty * NGRP + tg), 2), pl.ds(2 * me, 2)
            remote(src.at[theirs], dst.at[mine], sems, {"seq": ty, "grp": tg}).start()

    here = {"seq": ys[1]}
    rest = pl.ds(0, NDEV - 1)
    q_all = remote(qall.at[pl.ds(0, NGRP - 1)], qall.at[pl.ds(0, NGRP - 1)], q_sem, here)
    both = pl.ds(0, 2 * (NDEV - 1))
    k_all = remote(send_k.at[both], arr_k.at[both], k_sem, here)
    v0_all = remote(send_v0.at[both], arr_v0.at[both], v0_sem, here)
    v1_all = remote(send_v1.at[both], arr_v1.at[both], v1_sem, here)
    p_all = remote(pmsg.at[rest], part.at[rest], p_sem, here)
    s_all = remote(stat.at[rest], stat.at[rest], s_sem, here)
    a_all = remote(att.at[rest], att.at[rest], a_sem, here)
    z_all = remote(pout.at[pl.ds(0, NTP - 1)], zbuf.at[pl.ds(0, NTP - 1)], z_sem, here)

    keys_in.wait()
    vals_in.start()
    w_in.start()
    ahead = 6
    for offset in PEERS[:ahead]:
        pick_keys(0, *peer(offset))
    pl.semaphore_wait(barrier, NDEV - 1 + jnp.where(above, 1, 0) + jnp.where(below, 1, 0))
    for k in range(1, NGRP):
        remote(q_ref, qall.at[g], q_sem, {"grp": (g + k) % NGRP}).start()
    for i, offset in enumerate(PEERS):
        if i + ahead < len(PEERS):
            pick_keys(0, *peer(PEERS[i + ahead]))
        send_keys(0, *peer(offset))
    pick_keys(0, y, g)
    for offset in PEERS + [(0, 0, 0)]:
        pick_keys(1, *peer(offset))
    for offset in PEERS[:12]:
        send_keys(1, *peer(offset))
    vals_in.wait()
    lax.fori_loop(0, NDEV, pick_values, 0)
    scales_out.wait()
    lens_in.wait()
    q_all.wait_recv()

    lane1 = lax.broadcasted_iota(jnp.int32, (1, BLK), 1)

    def attend(gg, carry):
        q = qall[gg]
        scores, masks, key_scales, value_scales = [], [], [], []
        for n in range(8):
            t, r = (n // 2) * NGRP + gg, n % 2
            found_at = code_of(n // 2, gg, r)
            slot, row, column = (found_at >> 6) & 63, (found_at >> 5) & 1, (n // 2) * 32 + (found_at & 31)
            keys = send_k[2 * t + r]
            s = lax.dot_general(q, keys, (((1,), (1,)), ((), ())), preferred_element_type=jnp.float32)
            s = s * (scal[0, slot] * ROOT)
            value_scales.append(scal[1, slot])
            key_scales.append(scal[0, slot])
            limit = jnp.where((row16 >> 3) == row, lens[2 * gg + row] - column * BLK, 0)
            live = lane16 < limit
            scores.append(jnp.where(live, s, ABSENT))
            masks.append(live)
        top = functools.reduce(jnp.maximum, scores)
        peak = jnp.max(top, axis=1, keepdims=True)
        total = jnp.zeros((16, BLK), jnp.float32)
        acc = jnp.zeros((16, BLK), jnp.float32)
        for n in range(8):
            t, r = (n // 2) * NGRP + gg, n % 2
            weight = jnp.where(masks[n], jnp.exp(scores[n] - peak), 0.0)
            total = total + weight
            scaled = (weight * value_scales[n]).astype(jnp.bfloat16)
            values = jnp.concatenate([send_v0[2 * t + r], send_v1[2 * t + r]], axis=0)
            acc = acc + jnp.dot(scaled, values, preferred_element_type=jnp.float32)
        denom = jnp.sum(total, axis=1, keepdims=True)
        line = jnp.where(lane16 == row16, peak, jnp.where(lane16 == row16 + 16, denom, 0.0))
        line = jnp.sum(line, axis=0, keepdims=True)
        for n in range(8):
            line = jnp.where(lane1 == 32 + 2 * n, key_scales[n], line)
            line = jnp.where(lane1 == 33 + 2 * n, value_scales[n], line)
        smsg[gg] = line
        for qq in range(NSEQ):
            pmsg[qq * NGRP + gg] = acc[4 * qq : 4 * qq + 4].astype(jnp.bfloat16)
        return carry

    lax.fori_loop(0, NGRP, attend, 0)

    for offset in PEERS:
        ty, tg = peer(offset)
        remote(smsg.at[tg], stat.at[me], s_sem, {"seq": ty, "grp": tg}).start()
        remote(pmsg.at[ty * NGRP + tg], part.at[me], p_sem, {"seq": ty, "grp": tg}).start()
    part[me] = pmsg[me]
    stat[me] = smsg[g]
    for offset in PEERS[12:]:
        send_keys(1, *peer(offset))
    s_all.wait_recv()
    p_all.wait_recv()

    lines = jnp.broadcast_to(stat[...], (NDEV, 4, BLK))
    row = lax.broadcasted_iota(jnp.int32, (NDEV, 4, BLK), 1) + 4 * y
    lane = lax.broadcasted_iota(jnp.int32, (NDEV, 4, BLK), 2)
    peaks = jnp.sum(jnp.where(lane == row, lines, 0.0), axis=2, keepdims=True)
    sums = jnp.sum(jnp.where(lane == row + 16, lines, 0.0), axis=2, keepdims=True)
    peak = jnp.max(peaks, axis=0, keepdims=True)
    factor = jnp.exp(peaks - peak)
    denom = jnp.sum(sums * factor, axis=0)
    numer = jnp.sum(part[...].astype(jnp.float32) * factor, axis=0)
    rows = (numer / denom).astype(jnp.bfloat16)
    amsg[...] = rows
    att[(y % 2) * 16 + g * 2 + y // 2] = rows

    for offset in PEERS:
        ty, tg = peer(offset)
        remote(amsg, att.at[(y % 2) * 16 + g * 2 + y // 2], a_sem, {"seq": ty, "grp": tg}).start()
    send_values(send_v0, arr_v0, v0_sem)
    send_values(send_v1, arr_v1, v1_sem)
    for sent, arrived in ((send_k, arr_k), (send_v0, arr_v0), (send_v1, arr_v1)):
        arrived[pl.ds(2 * me, 2)] = sent[pl.ds(2 * me, 2)]
    wide = lax.broadcasted_iota(jnp.int32, (8, BLK), 1)
    first = pltpu.roll(jnp.broadcast_to(table[pl.ds(2 * g, 1), :], (8, BLK)), (BLK - 32 * y) % BLK, 1)
    second = pltpu.roll(jnp.broadcast_to(table[pl.ds(2 * g + 1, 1), :], (8, BLK)), (BLK + 32 - 32 * y) % BLK, 1)
    own = jnp.where(wide < 32, first, second)[0:1]
    across = jnp.broadcast_to(own, (BLK, BLK))
    down = across.T
    inside = lax.broadcasted_iota(jnp.int32, (BLK, BLK), 0) < 64
    before = inside & ((down >> 6) == (across >> 6)) & (down < across)
    rank = jnp.sum(before.astype(jnp.int32), axis=0, keepdims=True)
    place_v[...] = ((own >> 6) * 2 + rank) & 63
    place_in.start()
    owner = lax.broadcasted_iota(jnp.int32, (NDEV, BLK), 0)
    hot = (owner == (own >> 6)).astype(jnp.float32).astype(jnp.bfloat16)
    flat = stat[...].reshape(NDEV, BLK).T.astype(jnp.bfloat16)
    picked = jnp.dot(flat, hot, preferred_element_type=jnp.float32)
    depth = lax.broadcasted_iota(jnp.int32, (BLK, BLK), 0)
    for kv in range(2):
        line = jnp.where(depth == 32 + 4 * y + 2 * rank + kv, picked, 0.0)
        line = jnp.sum(line, axis=0, keepdims=True).astype(jnp.bfloat16)
        scale_out[0, kv : kv + 1, :] = line[:, 0:32]
        scale_out[1, kv : kv + 1, :] = line[:, 32:64]
    @pl.when(below)
    def _():
        pl.semaphore_wait(climb, 1)

    @pl.when(above)
    def _():
        pl.semaphore_signal(climb, inc=1, device_id={"tp": z + 1}, device_id_type=MESH)
        pl.semaphore_wait(descend, 1)

    @pl.when(below)
    def _():
        pl.semaphore_signal(descend, inc=1, device_id={"tp": z - 1}, device_id_type=MESH)

    w_in.wait()
    a_all.wait_recv()
    attended[...] = att[...].astype(jnp.float32)

    total = jnp.zeros((16, 256), jnp.float32)
    for h in range(8):
        lhs = attended[pl.ds((h // 4) * 16, 16), h % 4, :].astype(jnp.bfloat16)
        total = total + jnp.dot(lhs, w[pl.ds(h * BLK, BLK), :], preferred_element_type=jnp.float32)
    for k in range(NTP):
        pout[k] = total[2 * k : 2 * k + 2]

    for k in range(1, NTP):
        tz = (z + k) % NTP
        remote(pout.at[tz], zbuf.at[z], z_sem, {"tp": tz}).start()
    zbuf[z] = pout[z]
    z_all.wait_recv()
    out_ref[...] = jnp.sum(zbuf[...], axis=0).astype(jnp.bfloat16)

    place_in.wait()

    def settle(arrived, start, length):
        def body(p, carry):
            out[p, pl.ds(start, length), :] = arrived[place[0, p]]
            return carry

        lax.fori_loop(0, 64, body, 0, unroll=True)

    k_all.wait_recv()
    settle(arr_k, 0, BLK)
    v0_all.wait_recv()
    settle(arr_v0, BLK, HALF)
    for phase in (q_all, s_all, p_all, a_all, z_all, k_all, v0_all, v1_all):
        phase.wait_send()
    v1_all.wait_recv()
    settle(arr_v1, BLK + HALF, HALF)


def write_kernel(cache, summed, scales, out, out_sum, out_scales, sem):
    copies = [
        pltpu.make_async_copy(cache, out, sem.at[0]),
        pltpu.make_async_copy(summed, out_sum, sem.at[1]),
        pltpu.make_async_copy(scales, out_scales, sem.at[2]),
    ]
    for copy in copies:
        copy.start()
    for copy in copies:
        copy.wait()


def per_device(queries, cache_pool, block_scale, block_table, lengths, output_weight):
    vmem = pl.BlockSpec(memory_space=pltpu.VMEM)
    hbm = pl.BlockSpec(memory_space=pltpu.HBM)
    dma = pltpu.SemaphoreType.DMA
    cache, summed, scales = pl.pallas_call(
        exchange_kernel,
        out_shape=(
            jax.ShapeDtypeStruct((64, 256, BLK), jnp.bfloat16),
            jax.ShapeDtypeStruct((2, 256), jnp.bfloat16),
            jax.ShapeDtypeStruct((2, 2, 32), jnp.bfloat16),
        ),
        in_specs=[hbm] * 6,
        out_specs=(vmem, vmem, vmem),
        scratch_shapes=[
            pltpu.VMEM((16, BLK), jnp.int32),
            pltpu.VMEM((2, 64), jnp.bfloat16),
            pltpu.VMEM((16, BLK), jnp.int32),
            pltpu.VMEM((2, 64), jnp.float32),
            pltpu.SMEM((16, BLK), jnp.int32),
            pltpu.SMEM((2, 64), jnp.float32),
            pltpu.SMEM((16,), jnp.int32),
            pltpu.VMEM((1, BLK), jnp.int32),
            pltpu.SMEM((1, BLK), jnp.int32),
            pltpu.VMEM((64, BLK, BLK), jnp.bfloat16),
            pltpu.VMEM((64, BLK, BLK), jnp.bfloat16),
            pltpu.VMEM((64, BLK, BLK), jnp.bfloat16),
            pltpu.VMEM((64, HALF, BLK), jnp.bfloat16),
            pltpu.VMEM((64, HALF, BLK), jnp.bfloat16),
            pltpu.VMEM((64, BLK, BLK), jnp.bfloat16),
            pltpu.VMEM((64, HALF, BLK), jnp.bfloat16),
            pltpu.VMEM((64, HALF, BLK), jnp.bfloat16),
            pltpu.VMEM((16, BLK), jnp.bfloat16),
            pltpu.VMEM((NGRP, 16, BLK), jnp.bfloat16),
            pltpu.VMEM((1024, 256), jnp.bfloat16),
            pltpu.VMEM((NDEV, 4, BLK), jnp.bfloat16),
            pltpu.VMEM((NDEV, 4, BLK), jnp.bfloat16),
            pltpu.VMEM((NGRP, 1, BLK), jnp.float32),
            pltpu.VMEM((NDEV, 1, BLK), jnp.float32),
            pltpu.VMEM((4, BLK), jnp.bfloat16),
            pltpu.VMEM((NDEV, 4, BLK), jnp.bfloat16),
            pltpu.VMEM((NDEV, 4, BLK), jnp.float32),
            pltpu.VMEM((NTP, 2, 256), jnp.float32),
            pltpu.VMEM((NTP, 2, 256), jnp.float32),
            pltpu.SemaphoreType.REGULAR, pltpu.SemaphoreType.REGULAR,
            dma((10,)), dma((2,)), dma((2,)), dma((2,)), dma((2,)), dma((2,)), dma((2,)), dma((2,)), dma((2,)),
        ],
        compiler_params=pltpu.CompilerParams(
            collective_id=0, has_side_effects=True, vmem_limit_bytes=24 << 20
        ),
    )(*(
        pltpu.with_memory_space_constraint(operand, pltpu.HBM)
        for operand in (
            block_table, lengths, block_scale.reshape(64, 2).T, cache_pool.reshape(64, 256, BLK),
            queries.reshape(16, BLK), output_weight,
        )
    ))
    decode_cache, attention_output, decode_scale = pl.pallas_call(
        write_kernel,
        out_shape=(
            jax.ShapeDtypeStruct((64, 256, BLK), jnp.bfloat16),
            jax.ShapeDtypeStruct((2, 256), jnp.bfloat16),
            jax.ShapeDtypeStruct((2, 2, 32), jnp.bfloat16),
        ),
        in_specs=[vmem, vmem, vmem],
        out_specs=(hbm, hbm, hbm),
        scratch_shapes=[dma((3,))],
        compiler_params=pltpu.CompilerParams(vmem_limit_bytes=12 << 20),
    )(cache, summed, scales)
    return (
        attention_output,
        decode_cache.reshape(2, 32, 1, 2, BLK, BLK),
        decode_scale.transpose(0, 2, 1).reshape(2, 32, 1, 2),
    )


def solution(mesh):
    placed = (
        P("grp", "tp", None),
        P(("seq", "grp"), "tp", None, None, None),
        P(("seq", "grp"), "tp", None),
        P(),
        P(),
        P("tp", ("seq", "grp")),
    )
    return jax.shard_map(
        per_device,
        mesh=mesh,
        in_specs=placed,
        out_specs=(
            P("tp", ("seq", "grp")),
            P("grp", "seq", "tp", None, None, None),
            P("grp", "seq", "tp", None),
        ),
        check_vma=False,
    )
```
